256 devices in a mesh: rows: 128 (over y, z, x), cols: 2 (over core).
Axes of the slice: x: 4, y: 4, z: 8, core: 2. Of those that a mesh axis runs over, the one named last changes fastest.
Arguments:
- rhs: float32 [2, 768, 49152], P('cols', 'rows'), may hold values from -6 to 6
- pattern: int32 [384, 2], P(None, 'cols'), may hold values 0 or 1
- front_blocks: int32 [128, 4], replicated, may hold values from 0 to 383, as said below
- front_slot: int32 [128], replicated, may hold values from 0 to 255, as said below
- pivot_inverse: float32 [256, 256, 256], P('rows'), may hold values from -0.375 to 0.375
- update_factor: float32 [256, 256, 256], P('rows'), may hold values from -0.375 to 0.375
Outputs:
- solution: float32 [2, 768, 49152], P('cols', 'rows')
The draws below stay inside these ranges and needn't reach their ends.
Inputs may be any that keep to these rules, and one draw needn't show every extreme that they name: `front_blocks`: columns 0 and 1 together name every row block that is no contribution block exactly once; columns 2 and 3 of a front are two different blocks, never a pivot block of any front. `front_slot`: all different; slot s belongs to index s // 2 of rows; some index holds 2 fronts in every draw; slots that no front names are unused.
All inputs are finite; a program needn't handle non-finite values. No bound on the sum of `pattern` on one device may be relied on, other than what follows from the above.
Results may differ from the reference program's by a relative error of at most 0.0001.
Values sent between devices are 32-bit elements; how exact they have to be, the bound alone decides.
A program may use at most 64 MiB of HBM per device.

```python
import jax
import jax.numpy as jnp
from jax import lax

BLOCK = 128
PIV = 256
SLOT_DEV = 2
FRONTS = 128
SLOTS = 256
RB = 384
NROWS = 49152
GROUPS = 2
GCOLS = 768


def draw_front_blocks(key, part):
    shuffled = jax.random.permutation(jax.random.fold_in(key, 11), RB).astype(jnp.int32)
    pivots = shuffled[:2 * FRONTS].reshape(FRONTS, 2)
    separators = shuffled[2 * FRONTS:]
    first_sep = jax.random.randint(jax.random.fold_in(key, 12), (FRONTS,), 0, FRONTS).astype(jnp.int32)
    stride_draw = jax.random.randint(jax.random.fold_in(key, 13), (FRONTS,), 1, FRONTS).astype(jnp.int32)
    second_sep = (first_sep + stride_draw) % FRONTS
    return jnp.concatenate([pivots, separators[first_sep][:, None], separators[second_sep][:, None]], axis=1).astype(jnp.int32)


def draw_front_slot(key, part):
    shuffled = jax.random.permutation(jax.random.fold_in(key, 21), SLOTS).astype(jnp.int32)
    chosen = shuffled[:FRONTS]
    leading = chosen[0]
    partner = leading - leading % SLOT_DEV + (leading % SLOT_DEV + 1) % SLOT_DEV
    displaced = chosen[1]
    chosen = jnp.where(chosen == partner, displaced, chosen)
    chosen = chosen.at[1].set(partner)
    return chosen.astype(jnp.int32)


def set_ends(entries, rng, low, largest):
    extent = entries.shape
    place = [jax.random.randint(jax.random.fold_in(rng, axis), (), 0, extent[axis]) for axis in range(len(extent))]
    entries = entries.at[tuple(place)].set(low)
    longest = extent.index(max(extent))
    place[longest] = (place[longest] + 1) % extent[longest]
    return entries.at[tuple(place)].set(largest)


def steps_of(stream_key, extent, pieces, smallest, high):
    def one(dim, shards_of):
        steps = jax.random.uniform(jax.random.fold_in(jax.random.fold_in(stream_key, 6), dim), (shards_of,), jnp.float32, smallest / len(pieces), high / len(pieces))
        return jnp.repeat(jnp.exp(steps), extent[dim] // shards_of).reshape((-1,) + (1,) * (len(extent) - dim - 1))

    factor_of = one(*pieces[0])
    for cut in pieces[1:]:
        factor_of = factor_of * one(*cut)
    return factor_of


def centred(stream_key, shape, width, reach, pieces=(), kind=jnp.bfloat16):
    factor_of = steps_of(stream_key, shape, pieces, -0.22, 0.18) if pieces else 1.0
    array = jax.random.normal(stream_key, shape, jnp.float32) * width * factor_of
    return jnp.minimum(jnp.maximum(array, -reach), reach).astype(kind)


def setup_inputs(seed: int = 0) -> dict:
    seeds = jax.random.split(jax.random.key(seed), 7)
    return {
        "rhs": centred(seeds[0], (GROUPS, GCOLS, NROWS), 1.0, 6.0, ((0, 2), (1, 128)), jnp.float32),
        "pattern": set_ends((jax.random.randint(seeds[1], (RB, GROUPS), 0, 4) < 3).astype(jnp.int32), jax.random.fold_in(seeds[1], 1), 0, 1),
        "front_blocks": draw_front_blocks(jax.random.fold_in(seeds[6], 71), 0),
        "front_slot": draw_front_slot(jax.random.fold_in(seeds[6], 71), 0),
        "pivot_inverse": centred(seeds[4], (SLOTS, PIV, PIV), PIV ** -0.5, 0.375, ((0, 128),), jnp.float32),
        "update_factor": centred(seeds[5], (SLOTS, PIV, PIV), PIV ** -0.5, 0.375, ((0, 128),), jnp.float32),
    }


def reference(rhs, pattern, front_blocks, front_slot, pivot_inverse, update_factor):
    offsets = jnp.arange(BLOCK, dtype=jnp.int32)
    rows_of = (front_blocks[:, :, None] * BLOCK + offsets[None, None, :]).reshape(FRONTS, 4 * BLOCK).astype(jnp.int32)
    row_mask = jnp.repeat(pattern.astype(jnp.float32), BLOCK, axis=0)
    masked = rhs * jnp.transpose(row_mask)[:, None, :]
    strict_lower = jnp.tril(jnp.ones((PIV, PIV), jnp.float32), -1)
    identity = jnp.eye(PIV, dtype=jnp.float32)

    def one_front(result, front_index):
        rows = rows_of[front_index]
        slot_index = front_slot[front_index]
        pivots = jnp.take(masked, rows[:PIV], axis=2)
        inverse = identity + strict_lower * pivot_inverse[slot_index]
        solved = jnp.einsum("gcj,ij->gci", pivots, inverse, precision=lax.Precision.HIGHEST)
        update = jnp.einsum("gcj,ij->gci", solved, update_factor[slot_index], precision=lax.Precision.HIGHEST)
        result = result.at[:, :, rows[:PIV]].set(solved)
        result = result.at[:, :, rows[PIV:]].add(-update)
        return result, None

    result, _ = lax.scan(one_front, masked, jnp.arange(FRONTS, dtype=jnp.int32))
    return result
```

```python
import functools

import jax
import jax.numpy as jnp
from jax import lax
from jax.experimental import pallas as pl
from jax.experimental.pallas import tpu as pltpu
from jax.sharding import PartitionSpec as P

BLOCK = 128
PIV = 256
NX, NY, NZ = 4, 4, 8
PLANE = NX * NY
SLOT_DEV = 2
PAIRS = NZ
RING_SLOTS = NZ * SLOT_DEV
COLS = 6
MSG = COLS * 4
PACKED = 768
MESH = pl.DeviceIdType.MESH
PEERS = (
    (0, 1), (1, 0), (0, 3), (3, 0), (1, 1), (3, 3), (1, 3), (3, 1),
    (0, 2), (2, 0), (1, 2), (2, 1), (3, 2), (2, 3), (2, 2),
)


def nt(a, b):
    return lax.dot_general(a, b, (((1,), (1,)), ((), ())), preferred_element_type=jnp.float32)


def nn(a, b):
    return lax.dot_general(a, b, (((1,), (0,)), ((), ())), preferred_element_type=jnp.float32)


def split(v):
    high = v.astype(jnp.bfloat16)
    low = (v - high.astype(jnp.float32)).astype(jnp.bfloat16)
    return high, low


def product(dot, x, w):
    xh, xl = split(x)
    wh, wl = split(w)
    both = dot(jnp.concatenate([xh, xl], axis=0), wh)
    n = x.shape[0]
    return both[:n] + (both[n:] + dot(xh, wl))


def slot_place(slot, z):
    dev = lax.div(slot, SLOT_DEV)
    sl = lax.rem(slot, SLOT_DEV)
    ring = lax.div(dev, NX * NZ) * NX + lax.rem(dev, NX)
    zq = lax.rem(lax.div(dev, NX), NZ)
    delta = lax.rem(z - zq + NZ, NZ)
    near = jnp.minimum(delta, NZ - delta)
    above = (delta > NZ // 2).astype(jnp.int32)
    edge = jnp.logical_or(delta == 0, delta == NZ // 2)
    pair = jnp.where(delta == 0, 0, jnp.where(delta == NZ // 2, PAIRS - 1, 2 * near - 1 + lax.rem(sl + above, 2)))
    return ring, pair, jnp.where(edge, sl, above)


def prepare_kernel(slots, blocks, pattern, rhs, send):
    z = lax.rem(lax.div(lax.axis_index("rows"), NX), NZ)
    send[...] = jnp.zeros_like(send)

    def one_front(f, carry):
        ring, pair, a = slot_place(slots[f], z)
        for h in range(2):
            b = blocks[h, f]
            on = pattern[b].astype(jnp.float32)
            send[pair, ring, pl.ds(2 * a + h, COLS, stride=4), :] = rhs[:, b, :] * on
        return carry

    lax.fori_loop(0, slots.shape[0], one_front, 0, unroll=4)


def prepare(slots, blocks, pattern, rhs):
    vmem = pl.BlockSpec(memory_space=pltpu.VMEM)
    smem = pl.BlockSpec(memory_space=pltpu.SMEM)
    return pl.pallas_call(
        prepare_kernel,
        out_shape=jax.ShapeDtypeStruct((PAIRS, PLANE, MSG, BLOCK), jnp.float32),
        in_specs=[smem, smem, smem, vmem],
        out_specs=vmem,
        compiler_params=pltpu.CompilerParams(vmem_limit_bytes=16 * 1024 * 1024),
        name="prepare",
    )(slots, blocks, pattern, rhs)


def exchange_kernel(
    send, pinv, ufac, ret,
    fac, arr, back,
    ring_ss, ring_rs, core_ss, core_rs, out_ss, out_rs, ret_ss, ret_rs,
):
    r = lax.axis_index("rows")
    c = lax.axis_index("cols")
    x = lax.rem(r, NX)
    z = lax.rem(lax.div(r, NX), NZ)
    y = lax.div(r, NX * NZ)
    me = y * NX + x
    step_dir = 1 - 2 * c

    def chip(yy, zz, xx):
        return (yy * NZ + zz) * NX + xx

    def peer(dy, dx):
        return lax.rem(y + dy, NY), lax.rem(x + dx, NX)

    z_next = lax.rem(z + step_dir + NZ, NZ)
    z_prev = lax.rem(z - step_dir + NZ, NZ)

    barrier = pltpu.get_barrier_semaphore()
    for dy, dx in PEERS:
        py, px = peer(dy, dx)
        pl.semaphore_signal(barrier, inc=1, device_id=(chip(py, z, px), c), device_id_type=MESH)
    for zz in (z_next, z_prev):
        pl.semaphore_signal(barrier, inc=1, device_id=(chip(y, zz, x), c), device_id_type=MESH)
    pl.semaphore_signal(barrier, inc=1, device_id=(r, 1 - c), device_id_type=MESH)

    row = lax.broadcasted_iota(jnp.int32, (BLOCK, BLOCK), 0)
    col = lax.broadcasted_iota(jnp.int32, (BLOCK, BLOCK), 1)
    for s in range(SLOT_DEV):
        q = SLOT_DEV * z + s
        fac[q, 0:BLOCK, :] = jnp.where(
            row > col, pinv[s, :BLOCK, :BLOCK], pinv[s, BLOCK:, BLOCK:].T
        )
        fac[q, BLOCK : 2 * BLOCK, :] = pinv[s, BLOCK:, :BLOCK]
        fac[q, PIV : 2 * PIV, :] = ufac[s, :, :BLOCK]
        fac[q, 2 * PIV : 3 * PIV, :] = ufac[s, :, BLOCK:]

    pl.semaphore_wait(barrier, len(PEERS) + 3)

    def ring_copy(i):
        zs = lax.rem(z - step_dir * lax.div(i, 2) + NZ, NZ)
        q = SLOT_DEV * zs + lax.rem(i + c, 2)
        return pltpu.make_async_remote_copy(
            fac.at[q], fac.at[q], ring_ss.at[i], ring_rs.at[i],
            device_id=(chip(y, z_next, x), c), device_id_type=MESH,
        )

    def slot_from(i, cc):
        zs = lax.rem(z - (1 - 2 * cc) * (lax.div(i, 2) + 1) + NZ, NZ)
        return SLOT_DEV * zs + lax.rem(i + cc, 2)

    def core_copy(i, cc):
        q = slot_from(i, cc)
        return pltpu.make_async_remote_copy(
            fac.at[q], fac.at[q], core_ss.at[i], core_rs.at[i],
            device_id=(r, 1 - c), device_id_type=MESH,
        )

    def rows_at(ref, p, m):
        return ref.at[p, pl.ds(pl.multiple_of(m * MSG, 8), MSG), :]

    def start_out(p):
        for dy, dx in PEERS:
            py, px = peer(dy, dx)
            pltpu.make_async_remote_copy(
                send.at[p, py * NX + px], rows_at(arr, p, me), out_ss.at[p], out_rs.at[p],
                device_id=(chip(py, z, px), c), device_id_type=MESH,
            ).start()
        arr[p, pl.ds(pl.multiple_of(me * MSG, 8), MSG), :] = send[p, me]

    def start_back(t):
        for dy, dx in PEERS:
            py, px = peer(dy, dx)
            pltpu.make_async_remote_copy(
                rows_at(back, t, py * NX + px), rows_at(ret, t, me), ret_ss.at[t], ret_rs.at[t],
                device_id=(chip(py, z, px), c), device_id_type=MESH,
            ).start()
        pltpu.make_async_copy(rows_at(back, t, me), rows_at(ret, t, me), ret_rs.at[t]).start()

    def wait_bytes(ref, p, n, sem):
        view = ref.at[p, pl.ds(0, n * MSG), :]
        pltpu.make_async_copy(view, view, sem).wait()

    def solve(p, a, q):
        x0 = arr[p, pl.ds(2 * a, PLANE * COLS, stride=4), :]
        x1 = arr[p, pl.ds(2 * a + 1, PLANE * COLS, stride=4), :]
        merged = fac[q, 0:BLOCK, :]
        lower = jnp.where(row > col, merged, 0.0)
        upper = jnp.where(row < col, merged, 0.0)
        left = jnp.concatenate([lower, fac[q, BLOCK:PIV, :]], axis=0)
        first = product(nt, x0, left)
        y0 = x0 + first[:, :BLOCK]
        y1 = x1 + (first[:, BLOCK:] + product(nn, x1, upper))
        upd = product(nt, y0, fac[q, PIV : 2 * PIV, :]) + product(nt, y1, fac[q, 2 * PIV : 3 * PIV, :])
        t = 2 * p + a
        for h, v in enumerate((y0, y1, upd[:, :BLOCK], upd[:, BLOCK:])):
            back[t, pl.ds(h, PLANE * COLS, stride=4), :] = v
        start_back(t)

    ring_copy(0).start()
    ring_copy(1).start()
    start_out(0)

    def out_step(p, carry):
        start_out(p)
        return carry

    lax.fori_loop(1, PAIRS, out_step, 0)

    wait_bytes(arr, 0, PLANE - 1, out_rs.at[0])
    for a in range(2):
        solve(0, a, SLOT_DEV * z + a)

    def step(i, carry):
        ring_copy(i).wait_recv()

        @pl.when(i < PAIRS - 3)
        def _():
            ring_copy(i + 2).start()

        core_copy(i, c).start()
        wait_bytes(arr, i + 1, PLANE - 1, out_rs.at[i + 1])
        core_copy(i, 1 - c).wait_recv()
        solve(i + 1, 0, slot_from(i, 0))
        solve(i + 1, 1, slot_from(i, 1))
        return carry

    lax.fori_loop(0, PAIRS - 1, step, 0)

    def drain(i, carry):
        ring_copy(i).wait_send()
        core_copy(i, c).wait_send()
        return carry

    lax.fori_loop(0, PAIRS - 1, drain, 0)

    def drain_out(p, carry):
        wait_bytes(arr, p, PLANE - 1, out_ss.at[p])
        return carry

    lax.fori_loop(0, PAIRS, drain_out, 0)

    def drain_back(t, carry):
        wait_bytes(back, t, PLANE - 1, ret_ss.at[t])
        wait_bytes(back, t, PLANE, ret_rs.at[t])
        return carry

    lax.fori_loop(0, RING_SLOTS, drain_back, 0)


def exchange(send, pinv, ufac):
    vmem = pl.BlockSpec(memory_space=pltpu.VMEM)
    dma = pltpu.SemaphoreType.DMA
    return pl.pallas_call(
        exchange_kernel,
        out_shape=jax.ShapeDtypeStruct((RING_SLOTS, PLANE * MSG, BLOCK), jnp.float32),
        in_specs=[vmem, vmem, vmem],
        out_specs=pl.BlockSpec(memory_space=pl.ANY),
        scratch_shapes=[
            pltpu.VMEM((RING_SLOTS, PACKED, BLOCK), jnp.float32),
            pltpu.VMEM((PAIRS, PLANE * MSG, BLOCK), jnp.float32),
            pltpu.VMEM((RING_SLOTS, PLANE * MSG, BLOCK), jnp.float32),
            dma((PAIRS - 1,)), dma((PAIRS - 1,)), dma((PAIRS - 1,)), dma((PAIRS - 1,)),
            dma((PAIRS,)), dma((PAIRS,)), dma((RING_SLOTS,)), dma((RING_SLOTS,)),
        ],
        compiler_params=pltpu.CompilerParams(
            collective_id=0, has_side_effects=True, vmem_limit_bytes=40 * 1024 * 1024
        ),
        name="exchange",
    )(send, pinv, ufac)


def assemble_kernel(slots, blocks, pattern, rhs, ret, out):
    z = lax.rem(lax.div(lax.axis_index("rows"), NX), NZ)

    def mask_one(b, carry):
        on = pattern[b].astype(jnp.float32)
        out[:, b, :] = rhs[:, b, :] * on
        return carry

    lax.fori_loop(0, pattern.shape[0], mask_one, 0, unroll=8)

    def one_front(f, carry):
        ring, pair, a = slot_place(slots[f], z)
        at = (2 * pair + a) * PLANE + ring
        for h in range(4):
            b = blocks[h, f]
            v = ret[at, pl.ds(h, COLS, stride=4), :]
            if h < 2:
                out[:, b, :] = v
            else:
                out[:, b, :] = out[:, b, :] - v
        return carry

    lax.fori_loop(0, slots.shape[0], one_front, 0, unroll=2)


def assemble(slots, blocks, pattern, rhs, ret):
    vmem = pl.BlockSpec(memory_space=pltpu.VMEM)
    smem = pl.BlockSpec(memory_space=pltpu.SMEM)
    return pl.pallas_call(
        assemble_kernel,
        out_shape=jax.ShapeDtypeStruct(rhs.shape, jnp.float32),
        in_specs=[smem, smem, smem, vmem, vmem],
        out_specs=vmem,
        compiler_params=pltpu.CompilerParams(vmem_limit_bytes=16 * 1024 * 1024),
        name="assemble",
    )(slots, blocks, pattern, rhs, ret)


def on_device(rhs, pattern, front_blocks, front_slot, pivot_inverse, update_factor):
    shape = rhs.shape
    pattern = pattern.reshape(-1)
    blocks = front_blocks.T
    rhs = rhs.reshape(COLS, -1, BLOCK)
    send = prepare(front_slot, blocks, pattern, rhs)
    ret = exchange(send, pivot_inverse, update_factor)
    ret = ret.reshape(RING_SLOTS * PLANE, MSG, BLOCK)
    return assemble(front_slot, blocks, pattern, rhs, ret).reshape(shape)


def solution(mesh):
    return jax.shard_map(
        on_device,
        mesh=mesh,
        in_specs=(
            P("cols", "rows", None),
            P(None, "cols"),
            P(),
            P(),
            P("rows", None, None),
            P("rows", None, None),
        ),
        out_specs=P("cols", "rows", None),
        check_vma=False,
    )
```

```python
import functools

import jax
import jax.numpy as jnp
from jax import lax
from jax.experimental import pallas as pl
from jax.experimental.pallas import tpu as pltpu
from jax.sharding import PartitionSpec as P

BLOCK = 128
PIV = 256
NX, NY, NZ = 4, 4, 8
PLANE = NX * NY
SLOT_DEV = 2
PAIRS = NZ
RING_SLOTS = NZ * SLOT_DEV
COLS = 6
ROW_BLOCKS = 384
MSG = COLS * 4
NEAR = 2
PACKED = 768
MESH = pl.DeviceIdType.MESH
PEERS = (
    (0, 1), (1, 0), (0, 3), (3, 0), (1, 1), (3, 3), (1, 3), (3, 1),
    (0, 2), (2, 0), (1, 2), (2, 1), (3, 2), (2, 3), (2, 2),
)


def nt(a, b):
    return lax.dot_general(a, b, (((1,), (1,)), ((), ())), preferred_element_type=jnp.float32)


def nn(a, b):
    return lax.dot_general(a, b, (((1,), (0,)), ((), ())), preferred_element_type=jnp.float32)


def split(v):
    high = v.astype(jnp.bfloat16)
    low = (v - high.astype(jnp.float32)).astype(jnp.bfloat16)
    return high, low


def product(dot, x, w):
    xh, xl = split(x)
    wh, wl = split(w)
    both = dot(jnp.concatenate([xh, xl], axis=0), wh)
    n = x.shape[0]
    return both[:n] + (both[n:] + dot(xh, wl))


TIERS = (12, 14, 16)


def first_position(tier, p):
    if tier == 12:
        return max(p - 1, 0) if p < 3 else 2 * p - 4
    return max(2 * p - (16 - tier), 0)


def slot_in_sequence(o, z, ring):
    p, a = o // 2, o % 2
    i = p - 1
    reach = (i >> 1) + 1
    zs = jnp.where(p == 0, z, jnp.where(a == 0, z - reach, z + reach)) & (NZ - 1)
    sl = jnp.where(p == 0, a, (i + a) & 1)
    return (((ring >> 2) * NZ + zs) * NX + (ring & (NX - 1))) * SLOT_DEV + sl


def prepare_kernel(slots, blocks, mask, rhs, send, table, tier_ref, table_s, sem):
    z = lax.rem(lax.div(lax.axis_index("rows"), NX), NZ)
    shape = (RING_SLOTS, 128)
    o_of = lax.broadcasted_iota(jnp.int32, shape, 0)
    lane = lax.broadcasted_iota(jnp.int32, shape, 1)
    slot_of = slot_in_sequence(o_of, lane >> 4, lane & 15)

    def mark(f, occ):
        for k in range(8):
            occ = jnp.where(slot_of == slots[8 * f + k], 1, occ)
        return occ

    occ = lax.fori_loop(0, slots.shape[0] // 8, mark, jnp.zeros(shape, jnp.int32))
    used = occ > 0
    count = jnp.zeros((1, 128), jnp.int32)
    ranks = []
    last = {t: jnp.full((1, 128), -1, jnp.int32) for t in TIERS}
    places = {t: [] for t in TIERS}
    for o in range(RING_SLOTS):
        on = used[o : o + 1]
        ranks.append(jnp.where(on, count, 0))
        count = count + occ[o : o + 1]
        for t in TIERS:
            last[t] = jnp.where(on, jnp.maximum(last[t] + 1, first_position(t, o // 2)), last[t])
            places[t].append(jnp.where(on, last[t], 255))
    rank = jnp.concatenate(ranks, axis=0)
    fits = [jnp.max(last[t]) < t for t in TIERS]
    tier = jnp.where(fits[0], 0, jnp.where(fits[1], 1, 2))
    place = {t: jnp.concatenate(places[t], axis=0) for t in TIERS}
    place = jnp.where(tier == 0, place[TIERS[0]], jnp.where(tier == 1, place[TIERS[1]], place[TIERS[2]]))
    holds = jnp.zeros(shape, jnp.int32)
    for o in range(RING_SLOTS):
        holds = jnp.where(place[o : o + 1] == o_of, o, holds)
    table[...] = rank + (place << 8) + (holds << 16)
    tier_ref[0] = tier
    copy = pltpu.make_async_copy(table, table_s, sem)
    copy.start()
    send[...] = jnp.zeros_like(send)
    copy.wait()

    def one_front(f, carry):
        o, ring = sequence_of(slots[f], z)
        k = table_s[o, z * PLANE + ring] & 255
        for h in range(2):
            b = blocks[h, f]
            v = rhs[pl.ds(b, COLS, stride=ROW_BLOCKS), :] * mask[pl.ds(b, 1), :]
            send[k >> 1, ring, pl.ds(2 * (k & 1) + h, COLS, stride=4), :] = v
        return carry

    lax.fori_loop(0, slots.shape[0], one_front, 0, unroll=4)


def sequence_of(slot, z):
    sl = slot & 1
    ring = ((slot >> 6) << 2) + ((slot >> 1) & 3)
    delta = (z - (slot >> 3)) & (NZ - 1)
    near = jnp.minimum(delta, NZ - delta)
    above = jnp.where(delta > NZ // 2, 1, 0)
    o = 4 * near - 2 + 2 * (sl ^ above) + above
    o = jnp.where(delta == NZ // 2, 2 * (PAIRS - 1) + sl, o)
    return jnp.where(delta == 0, sl, o), ring


def prepare(slots, blocks, mask, rhs):
    vmem = pl.BlockSpec(memory_space=pltpu.VMEM)
    smem = pl.BlockSpec(memory_space=pltpu.SMEM)
    return pl.pallas_call(
        prepare_kernel,
        out_shape=(
            jax.ShapeDtypeStruct((PAIRS, PLANE, MSG, BLOCK), jnp.float32),
            jax.ShapeDtypeStruct((RING_SLOTS, 128), jnp.int32),
            jax.ShapeDtypeStruct((1,), jnp.int32),
        ),
        in_specs=[smem, smem, vmem, vmem],
        out_specs=(vmem, vmem, smem),
        scratch_shapes=[
            pltpu.SMEM((RING_SLOTS, 128), jnp.int32),
            pltpu.SemaphoreType.DMA,
        ],
        compiler_params=pltpu.CompilerParams(vmem_limit_bytes=16 * 1024 * 1024),
        name="prepare",
    )(slots, blocks, mask, rhs)


def exchange_kernel(
    tier, table, send, pinv, ufac, ret,
    fac, near, arr, res, back,
    ring_ss, ring_rs, core_ss, core_rs, out_ss, out_rs, ret_ss, ret_rs,
):
    r = lax.axis_index("rows")
    c = lax.axis_index("cols")
    x = lax.rem(r, NX)
    z = lax.rem(lax.div(r, NX), NZ)
    y = lax.div(r, NX * NZ)
    me = y * NX + x
    step_dir = 1 - 2 * c

    def chip(yy, zz, xx):
        return (yy * NZ + zz) * NX + xx

    def peer(dy, dx):
        return lax.rem(y + dy, NY), lax.rem(x + dx, NX)

    z_next = lax.rem(z + step_dir + NZ, NZ)
    z_prev = lax.rem(z - step_dir + NZ, NZ)

    barrier = pltpu.get_barrier_semaphore()
    for dy, dx in PEERS:
        py, px = peer(dy, dx)
        pl.semaphore_signal(barrier, inc=1, device_id=(chip(py, z, px), c), device_id_type=MESH)
    for zz in (z_next, z_prev):
        pl.semaphore_signal(barrier, inc=1, device_id=(chip(y, zz, x), c), device_id_type=MESH)
    pl.semaphore_signal(barrier, inc=1, device_id=(r, 1 - c), device_id_type=MESH)

    row = lax.broadcasted_iota(jnp.int32, (BLOCK, BLOCK), 0)
    col = lax.broadcasted_iota(jnp.int32, (BLOCK, BLOCK), 1)
    for s in range(SLOT_DEV):
        q = SLOT_DEV * z + s
        fac[q, 0:BLOCK, :] = jnp.where(
            row > col, pinv[s, :BLOCK, :BLOCK], pinv[s, BLOCK:, BLOCK:].T
        )
        fac[q, BLOCK : 2 * BLOCK, :] = pinv[s, BLOCK:, :BLOCK]
        fac[q, PIV : 2 * PIV, :] = ufac[s, :, :BLOCK]
        fac[q, 2 * PIV : 3 * PIV, :] = ufac[s, :, BLOCK:]

    pl.semaphore_wait(barrier, len(PEERS) + 3)

    def ring_copy(i):
        zs = lax.rem(z - step_dir * lax.div(i, 2) + NZ, NZ)
        q = SLOT_DEV * zs + lax.rem(i + c, 2)
        return pltpu.make_async_remote_copy(
            fac.at[q], fac.at[q], ring_ss.at[i], ring_rs.at[i],
            device_id=(chip(y, z_next, x), c), device_id_type=MESH,
        )

    def slot_from(i, cc):
        zs = lax.rem(z - (1 - 2 * cc) * (lax.div(i, 2) + 1) + NZ, NZ)
        return SLOT_DEV * zs + lax.rem(i + cc, 2)

    def core_copy(i, cc):
        q = slot_from(i, cc)
        return pltpu.make_async_remote_copy(
            fac.at[q], fac.at[q], core_ss.at[i], core_rs.at[i],
            device_id=(r, 1 - c), device_id_type=MESH,
        )

    def rows_at(ref, p, m):
        return ref.at[p, pl.ds(pl.multiple_of(m * MSG, 8), MSG), :]

    def start_out(p, into):
        for dy, dx in PEERS:
            py, px = peer(dy, dx)
            pltpu.make_async_remote_copy(
                send.at[p, py * NX + px], rows_at(into, p, me), out_ss.at[p], out_rs.at[p],
                device_id=(chip(py, z, px), c), device_id_type=MESH,
            ).start()
        into[p, pl.ds(pl.multiple_of(me * MSG, 8), MSG), :] = send[p, me]

    def start_back(t):
        for dy, dx in PEERS:
            py, px = peer(dy, dx)
            pltpu.make_async_remote_copy(
                rows_at(back, t, py * NX + px), rows_at(ret, t, me), ret_ss.at[t], ret_rs.at[t],
                device_id=(chip(py, z, px), c), device_id_type=MESH,
            ).start()
        pltpu.make_async_copy(rows_at(back, t, me), rows_at(ret, t, me), ret_rs.at[t]).start()

    def wait_bytes(ref, p, n, sem):
        view = ref.at[p, pl.ds(0, n * MSG), :]
        pltpu.make_async_copy(view, view, sem).wait()

    lane = z * PLANE + me

    def solve(o, q, data):
        k = table[o, lane] & 255
        data = data.at[k >> 1]
        second = (k & 1) == 1
        x0, x1 = (
            jnp.where(
                second,
                data[pl.ds(2 + h, PLANE * COLS, stride=4), :],
                data[pl.ds(h, PLANE * COLS, stride=4), :],
            )
            for h in range(2)
        )
        merged = fac[q, 0:BLOCK, :]
        lower = jnp.where(row > col, merged, 0.0)
        upper = jnp.where(row < col, merged, 0.0)
        left = jnp.concatenate([lower, fac[q, BLOCK:PIV, :]], axis=0)
        first = product(nt, x0, left)
        y0 = x0 + first[:, :BLOCK]
        y1 = x1 + (first[:, BLOCK:] + product(nn, x1, upper))
        upd = product(nt, y0, fac[q, PIV : 2 * PIV, :]) + product(nt, y1, fac[q, 2 * PIV : 3 * PIV, :])
        for h, v in enumerate((y0, y1, upd[:, :BLOCK], upd[:, BLOCK:])):
            res[o, pl.ds(h, PLANE * COLS, stride=4), :] = v

    def give_back(t):
        back[t] = res[table[t, lane] >> 16]
        start_back(t)

    ring_copy(0).start()
    ring_copy(1).start()
    for p in range(NEAR):
        start_out(p, near)

    def out_step(p, carry):
        start_out(p, arr)
        return carry

    lax.fori_loop(NEAR, tier // 2, out_step, 0)

    for p in range(NEAR):
        wait_bytes(near, p, PLANE - 1, out_rs.at[p])
    for a in range(2):
        solve(a, SLOT_DEV * z + a, near)
    if first_position(tier, 1) > 0:
        for t in range(first_position(tier, 1)):
            give_back(t)

    def advance(i):
        ring_copy(i).wait_recv()

        @pl.when(i < PAIRS - 3)
        def _():
            ring_copy(i + 2).start()

        core_copy(i, c).start()
        core_copy(i, 1 - c).wait_recv()

    advance(jnp.int32(0))
    for a in range(2):
        solve(2 + a, slot_from(jnp.int32(0), a), near)
    for t in range(first_position(tier, 1), first_position(tier, 2)):
        give_back(t)

    for p in range(NEAR):
        arr[p] = near[p]

    def arrive(p, carry):
        wait_bytes(arr, p, PLANE - 1, out_rs.at[p])
        return carry

    lax.fori_loop(NEAR, tier // 2, arrive, 0)

    def step(i, carry):
        advance(i)
        for a in range(2):
            solve(2 * i + 2 + a, slot_from(i, a), arr)
        p = i + 1
        if tier == 12:
            t = jnp.where(p < 3, p - 1, 2 * p - 4)
        else:
            t = 2 * p - (16 - tier)
        give_back(t)

        @pl.when(p >= (3 if tier == 12 else 0))
        def _():
            give_back(t + 1)

        return carry

    lax.fori_loop(1, PAIRS - 1, step, 0)

    def drain(i, carry):
        ring_copy(i).wait_send()
        core_copy(i, c).wait_send()
        return carry

    lax.fori_loop(0, PAIRS - 1, drain, 0)

    def drain_out(p, carry):
        wait_bytes(arr, p, PLANE - 1, out_ss.at[p])
        return carry

    lax.fori_loop(0, tier // 2, drain_out, 0)

    def drain_back(t, carry):
        wait_bytes(back, t, PLANE - 1, ret_ss.at[t])
        wait_bytes(back, t, PLANE, ret_rs.at[t])
        return carry

    lax.fori_loop(0, tier, drain_back, 0)


def exchange(tier, table, send, pinv, ufac):
    vmem = pl.BlockSpec(memory_space=pltpu.VMEM)
    dma = pltpu.SemaphoreType.DMA
    return pl.pallas_call(
        functools.partial(exchange_kernel, tier),
        out_shape=jax.ShapeDtypeStruct((RING_SLOTS, PLANE * MSG, BLOCK), jnp.float32),
        in_specs=[pl.BlockSpec(memory_space=pltpu.SMEM), vmem, vmem, vmem],
        out_specs=pl.BlockSpec(memory_space=pl.ANY),
        scratch_shapes=[
            pltpu.VMEM((RING_SLOTS, PACKED, BLOCK), jnp.float32),
            pltpu.VMEM((NEAR, PLANE * MSG, BLOCK), jnp.float32),
            pltpu.VMEM((PAIRS, PLANE * MSG, BLOCK), jnp.float32),
            pltpu.VMEM((RING_SLOTS, PLANE * MSG, BLOCK), jnp.float32),
            pltpu.VMEM((RING_SLOTS, PLANE * MSG, BLOCK), jnp.float32),
            dma((PAIRS - 1,)), dma((PAIRS - 1,)), dma((PAIRS - 1,)), dma((PAIRS - 1,)),
            dma((PAIRS,)), dma((PAIRS,)), dma((RING_SLOTS,)), dma((RING_SLOTS,)),
        ],
        compiler_params=pltpu.CompilerParams(
            collective_id=TIERS.index(tier), has_side_effects=True, vmem_limit_bytes=40 * 1024 * 1024
        ),
        name=f"exchange_{tier}",
    )(table, send, pinv, ufac)


def assemble_kernel(table, slots, blocks, mask, rhs, ret, out):
    z = lax.rem(lax.div(lax.axis_index("rows"), NX), NZ)
    for j in range(COLS):
        rows = pl.ds(j * ROW_BLOCKS, ROW_BLOCKS)
        out[rows, :] = rhs[rows, :] * mask[...]

    def one_front(f, carry):
        o, ring = sequence_of(slots[f], z)
        at = ((table[o, z * PLANE + ring] >> 8) & 255) * PLANE + ring
        for h in range(4):
            rows = pl.ds(blocks[h, f], COLS, stride=ROW_BLOCKS)
            v = ret[at, pl.ds(h, COLS, stride=4), :]
            if h < 2:
                out[rows, :] = v
            else:
                out[rows, :] = out[rows, :] - v
        return carry

    lax.fori_loop(0, slots.shape[0], one_front, 0, unroll=2)


def assemble(table, slots, blocks, mask, rhs, ret):
    vmem = pl.BlockSpec(memory_space=pltpu.VMEM)
    smem = pl.BlockSpec(memory_space=pltpu.SMEM)
    return pl.pallas_call(
        assemble_kernel,
        out_shape=jax.ShapeDtypeStruct(rhs.shape, jnp.float32),
        in_specs=[smem, smem, smem, vmem, vmem, vmem],
        out_specs=vmem,
        compiler_params=pltpu.CompilerParams(vmem_limit_bytes=16 * 1024 * 1024),
        name="assemble",
    )(table, slots, blocks, mask, rhs, ret)


def on_device(rhs, pattern, front_blocks, front_slot, pivot_inverse, update_factor):
    shape = rhs.shape
    mask = jnp.broadcast_to(pattern.astype(jnp.float32), (ROW_BLOCKS, BLOCK))
    blocks = front_blocks.T
    rhs = rhs.reshape(COLS * ROW_BLOCKS, BLOCK)
    send, table, tier = prepare(front_slot, blocks, mask, rhs)
    ret = lax.switch(
        tier[0], [functools.partial(exchange, t) for t in TIERS], table, send, pivot_inverse, update_factor
    )
    ret = ret.reshape(RING_SLOTS * PLANE, MSG, BLOCK)
    return assemble(table, front_slot, blocks, mask, rhs, ret).reshape(shape)


def solution(mesh):
    return jax.shard_map(
        on_device,
        mesh=mesh,
        in_specs=(
            P("cols", "rows", None),
            P(None, "cols"),
            P(),
            P(),
            P("rows", None, None),
            P("rows", None, None),
        ),
        out_specs=P("cols", "rows", None),
        check_vma=False,
    )
```

```python
import functools

import jax
import jax.numpy as jnp
from jax import lax
from jax.experimental import pallas as pl
from jax.experimental.pallas import tpu as pltpu
from jax.sharding import PartitionSpec as P

BLOCK = 128
PIV = 256
NX, NY, NZ = 4, 4, 8
PLANE = NX * NY
SLOT_DEV = 2
PAIRS = NZ
RING_SLOTS = NZ * SLOT_DEV
COLS = 6
ROW_BLOCKS = 384
MSG = COLS * 4
NEAR = 2
FAR = 6
PACKED = 768
MESH = pl.DeviceIdType.MESH
PEERS = (
    (0, 1), (1, 0), (0, 3), (3, 0), (1, 1), (3, 3), (1, 3), (3, 1),
    (0, 2), (2, 0), (1, 2), (2, 1), (3, 2), (2, 3), (2, 2),
)


def nt(a, b):
    return lax.dot_general(a, b, (((1,), (1,)), ((), ())), preferred_element_type=jnp.float32)


def nn(a, b):
    return lax.dot_general(a, b, (((1,), (0,)), ((), ())), preferred_element_type=jnp.float32)


def split(v):
    high = v.astype(jnp.bfloat16)
    low = (v - high.astype(jnp.float32)).astype(jnp.bfloat16)
    return high, low


def product(dot, x, w):
    xh, xl = split(x)
    wh, wl = split(w)
    both = dot(jnp.concatenate([xh, xl], axis=0), wh)
    n = x.shape[0]
    return both[:n] + (both[n:] + dot(xh, wl))


TIERS = (12, 14, 16)


def first_position(tier, o):
    p = o // 2
    last = o - 14 if p == PAIRS - 1 else 0
    if tier == 12:
        return (max(p - 1, 0) if p < 3 else 2 * p - 4) + last
    return max(2 * p - (16 - tier), 0) + last


def slot_in_sequence(o, z, ring):
    p, a = o >> 1, o & 1
    i = p - 1
    reach = (i >> 1) + 1
    edge = jnp.logical_or(p == 0, p == PAIRS - 1)
    zs = jnp.where(p == 0, z, jnp.where(a == 0, z - reach, z + reach)) & (NZ - 1)
    sl = jnp.where(edge, a, i & 1)
    zs = jnp.where(p == PAIRS - 1, z + NZ // 2, zs) & (NZ - 1)
    return (((ring >> 2) * NZ + zs) * NX + (ring & (NX - 1))) * SLOT_DEV + sl


def sequence_of(slot, z):
    sl = slot & 1
    ring = ((slot >> 6) << 2) + ((slot >> 1) & 3)
    delta = (z - (slot >> 3)) & (NZ - 1)
    below = delta < NZ // 2
    o = 4 * jnp.where(below, delta, NZ - delta) - 2 + 2 * sl + jnp.where(below, 0, 1)
    o = jnp.where(delta == NZ // 2, 2 * (PAIRS - 1) + sl, o)
    return jnp.where(delta == 0, sl, o), ring


def tables_kernel(slots_h, blocks_h, table, tier_ref, slots, blocks, sems):
    one = pltpu.make_async_copy(slots_h, slots, sems.at[0])
    two = pltpu.make_async_copy(blocks_h, blocks, sems.at[1])
    one.start()
    two.start()
    shape = (RING_SLOTS, 128)
    o_of = lax.broadcasted_iota(jnp.int32, shape, 0)
    lane = lax.broadcasted_iota(jnp.int32, shape, 1)
    slot_of = slot_in_sequence(o_of, lane >> 4, lane & 15)
    one.wait()
    two.wait()

    def mark(f, code):
        for k in range(8):
            g = 8 * f + k
            code = jnp.where(slot_of == slots[g], 1 + blocks[0, g] + (blocks[1, g] << 9), code)
        return code

    code = lax.fori_loop(0, slots.shape[0] // 8, mark, jnp.zeros(shape, jnp.int32))
    used = code > 0
    count = jnp.zeros((1, 128), jnp.int32)
    ranks = []
    last = {t: jnp.full((1, 128), -1, jnp.int32) for t in TIERS}
    places = {t: [] for t in TIERS}
    for o in range(RING_SLOTS):
        on = used[o : o + 1]
        ranks.append(jnp.where(on, count, 0))
        count = count + on.astype(jnp.int32)
        for t in TIERS:
            last[t] = jnp.where(on, jnp.maximum(last[t] + 1, first_position(t, o)), last[t])
            places[t].append(jnp.where(on, last[t], 255))
    fits = [jnp.max(last[t]) < t for t in TIERS]
    tier = jnp.where(fits[0], 0, jnp.where(fits[1], 1, 2))
    place = {t: jnp.concatenate(places[t], axis=0) for t in TIERS}
    place = jnp.where(tier == 0, place[TIERS[0]], jnp.where(tier == 1, place[TIERS[1]], place[TIERS[2]]))
    holds = jnp.zeros(shape, jnp.int32)
    by_rank = jnp.zeros(shape, jnp.int32)
    for o in range(RING_SLOTS):
        holds = jnp.where(place[o : o + 1] == o_of, o, holds)
        own = jnp.logical_and(used[o : o + 1], ranks[o] == o_of)
        by_rank = jnp.where(own, code[o : o + 1] - 1, by_rank)
    table[0:RING_SLOTS, :] = jnp.concatenate(ranks, axis=0) + (place << 8) + (holds << 16)
    table[RING_SLOTS : 2 * RING_SLOTS, :] = by_rank
    tier_ref[0] = tier


def make_tables(slots, blocks):
    hbm = pl.BlockSpec(memory_space=pltpu.HBM)
    return pl.pallas_call(
        tables_kernel,
        out_shape=(
            jax.ShapeDtypeStruct((2 * RING_SLOTS, 128), jnp.int32),
            jax.ShapeDtypeStruct((1,), jnp.int32),
        ),
        in_specs=[hbm, hbm],
        out_specs=(pl.BlockSpec(memory_space=pltpu.VMEM), pl.BlockSpec(memory_space=pltpu.SMEM)),
        scratch_shapes=[
            pltpu.SMEM(slots.shape, jnp.int32),
            pltpu.SMEM(blocks.shape, jnp.int32),
            pltpu.SemaphoreType.DMA((2,)),
        ],
        name="tables",
    )(slots, blocks)


def exchange_kernel(
    tier, table_h, pattern_h, rhs_h, pinv_h, ufac_h, ret, acc,
    table, pattern, rhs, pinv, ufac, mask, send, fac, near, arr, res, back, in_sems,
    ring_ss, ring_rs, core_ss, core_rs, out_ss, out_rs, ret_ss, ret_rs,
):
    r = lax.axis_index("rows")
    c = lax.axis_index("cols")
    x = lax.rem(r, NX)
    z = lax.rem(lax.div(r, NX), NZ)
    y = lax.div(r, NX * NZ)
    me = y * NX + x

    def chip(yy, zz, xx):
        return (yy * NZ + zz) * NX + xx

    def peer(dy, dx):
        return lax.rem(y + dy, NY), lax.rem(x + dx, NX)

    above = lax.rem(z + 1, NZ)
    below = lax.rem(z + NZ - 1, NZ)

    barrier = pltpu.get_barrier_semaphore()
    for dy, dx in PEERS:
        py, px = peer(dy, dx)
        pl.semaphore_signal(barrier, inc=1, device_id=(chip(py, z, px), c), device_id_type=MESH)
    for zz in (above, below):
        pl.semaphore_signal(barrier, inc=1, device_id=(chip(y, zz, x), c), device_id_type=MESH)
    pl.semaphore_signal(barrier, inc=1, device_id=(r, 1 - c), device_id_type=MESH)

    fetches = [
        pltpu.make_async_copy(src, dst, in_sems.at[k])
        for k, (src, dst) in enumerate(
            ((pinv_h, pinv), (ufac_h, ufac), (table_h, table), (pattern_h, pattern), (rhs_h, rhs))
        )
    ]
    for fetch in fetches:
        fetch.start()
    fetches[0].wait()
    fetches[1].wait()

    row = lax.broadcasted_iota(jnp.int32, (BLOCK, BLOCK), 0)
    col = lax.broadcasted_iota(jnp.int32, (BLOCK, BLOCK), 1)
    for s in range(SLOT_DEV):
        q = SLOT_DEV * z + s
        fac[q, 0:BLOCK, :] = jnp.where(
            row > col, pinv[s, :BLOCK, :BLOCK], pinv[s, BLOCK:, BLOCK:].T
        )
        fac[q, BLOCK : 2 * BLOCK, :] = pinv[s, BLOCK:, :BLOCK]
        fac[q, PIV : 2 * PIV, :] = ufac[s, :, :BLOCK]
        fac[q, 2 * PIV : 3 * PIV, :] = ufac[s, :, BLOCK:]

    pl.semaphore_wait(barrier, len(PEERS) + 3)

    half = pl.ds(pl.multiple_of(c * (PACKED // 2), PACKED // 2), PACKED // 2)

    def slot_at(i, d, away):
        zs = lax.rem(z - (1 - 2 * d) * (lax.div(i, 2) + away) + NZ, NZ)
        return SLOT_DEV * zs + lax.rem(i, 2)

    def slot_from(i, d):
        return slot_at(i, d, 1)

    def part(i, d):
        if i is not None and i >= FAR:
            at = c * (PACKED // 2) + d * (PACKED // 4)
            return pl.ds(pl.multiple_of(at, PACKED // 4), PACKED // 4)
        return half

    def ring_copy(i, d, far=None):
        q = slot_at(i, d, 0)
        view = fac.at[q, part(far, d), :]
        return pltpu.make_async_remote_copy(
            view, view, ring_ss.at[d, i], ring_rs.at[d, i],
            device_id=(chip(y, (above, below)[d], x), c), device_id_type=MESH,
        )

    def core_copy(i, d, far=None):
        view = fac.at[slot_from(i, d), part(far, d), :]
        return pltpu.make_async_remote_copy(
            view, view, core_ss.at[d, i], core_rs.at[d, i],
            device_id=(r, 1 - c), device_id_type=MESH,
        )

    lane = z * PLANE + me

    def pack(p):
        def one(m, carry):
            for a in range(2):
                code = table[RING_SLOTS + 2 * p + a, z * PLANE + m]
                for h, b in enumerate((code & 511, code >> 9)):
                    v = rhs[pl.ds(b, COLS, stride=ROW_BLOCKS), :] * mask[pl.ds(b, 1), :]
                    send[p, m, pl.ds(2 * a + h, COLS, stride=4), :] = v
            return carry

        lax.fori_loop(0, PLANE, one, 0, unroll=2)

    def rows_at(ref, p, m):
        return ref.at[p, pl.ds(pl.multiple_of(m * MSG, 8), MSG), :]

    def start_out(p, into):
        for dy, dx in PEERS:
            py, px = peer(dy, dx)
            pltpu.make_async_remote_copy(
                send.at[p, py * NX + px], rows_at(into, p, me), out_ss.at[p], out_rs.at[p],
                device_id=(chip(py, z, px), c), device_id_type=MESH,
            ).start()
        into[p, pl.ds(pl.multiple_of(me * MSG, 8), MSG), :] = send[p, me]

    def start_back(t):
        for dy, dx in PEERS:
            py, px = peer(dy, dx)
            pltpu.make_async_remote_copy(
                rows_at(back, t, py * NX + px), rows_at(ret, t, me), ret_ss.at[t], ret_rs.at[t],
                device_id=(chip(py, z, px), c), device_id_type=MESH,
            ).start()
        pltpu.make_async_copy(rows_at(back, t, me), rows_at(ret, t, me), ret_rs.at[t]).start()

    def wait_bytes(ref, p, n, sem):
        view = ref.at[p, pl.ds(0, n * MSG), :]
        pltpu.make_async_copy(view, view, sem).wait()

    def solve(o, q, data):
        k = table[o, lane] & 255
        data = data.at[k >> 1]
        second = (k & 1) == 1
        x0, x1 = (
            jnp.where(
                second,
                data[pl.ds(2 + h, PLANE * COLS, stride=4), :],
                data[pl.ds(h, PLANE * COLS, stride=4), :],
            )
            for h in range(2)
        )
        merged = fac[q, 0:BLOCK, :]
        lower = jnp.where(row > col, merged, 0.0)
        upper = jnp.where(row < col, merged, 0.0)
        left = jnp.concatenate([lower, fac[q, BLOCK:PIV, :]], axis=0)
        first = product(nt, x0, left)
        y0 = x0 + first[:, :BLOCK]
        y1 = x1 + (first[:, BLOCK:] + product(nn, x1, upper))
        upd = product(nt, y0, fac[q, PIV : 2 * PIV, :]) + product(nt, y1, fac[q, 2 * PIV : 3 * PIV, :])
        for h, v in enumerate((y0, y1, upd[:, :BLOCK], upd[:, BLOCK:])):
            res[o, pl.ds(h, PLANE * COLS, stride=4), :] = v

    def give_back(t):
        back[t] = res[table[t, lane] >> 16]
        start_back(t)

    for i in range(2):
        for d in range(2):
            ring_copy(jnp.int32(i), d).start()
    fetches[3].wait()
    for k in range(ROW_BLOCKS // BLOCK):
        on = pattern[:, k * BLOCK : (k + 1) * BLOCK].astype(jnp.float32)
        mask[k * BLOCK : (k + 1) * BLOCK, :] = jnp.broadcast_to(on, (BLOCK, BLOCK)).T
    fetches[2].wait()
    fetches[4].wait()
    for p in range(NEAR):
        pack(p)
        start_out(p, near)

    def out_step(p, carry):
        pack(p)
        start_out(p, arr)
        return carry

    lax.fori_loop(NEAR, tier // 2, out_step, 0)

    def init(k, carry):
        on = mask[pl.ds(pl.multiple_of(8 * k, 8), 8), :]
        for j in range(COLS):
            v = rhs[pl.ds(pl.multiple_of(j * ROW_BLOCKS + 8 * k, 8), 8), :] * on
            acc[pl.ds(64 * k + j, 8, stride=8), :] = v
        return carry

    lax.fori_loop(0, ROW_BLOCKS // 8, init, 0, unroll=2)

    for p in range(NEAR):
        wait_bytes(near, p, PLANE - 1, out_rs.at[p])
    for a in range(2):
        solve(a, SLOT_DEV * z + a, near)
    for t in range(first_position(tier, 2)):
        give_back(t)

    def advance(i):
        for d in range(2):
            ring_copy(i, d).wait_recv()

            @pl.when(i < FAR - 2)
            def _():
                ring_copy(i + 2, d).start()

            @pl.when(i >= FAR - 2)
            def _():
                ring_copy(i + 2, d, FAR).start()

            core_copy(i, d).start()
        for d in range(2):
            core_copy(i, d).wait_recv()

    advance(jnp.int32(0))
    for a in range(2):
        solve(2 + a, slot_from(jnp.int32(0), a), near)
    for t in range(first_position(tier, 2), first_position(tier, 4)):
        give_back(t)

    for p in range(NEAR):
        arr[p] = near[p]

    def arrive(p, carry):
        wait_bytes(arr, p, PLANE - 1, out_rs.at[p])
        return carry

    lax.fori_loop(NEAR, tier // 2, arrive, 0)

    def step(i, carry):
        advance(i)
        for a in range(2):
            solve(2 * i + 2 + a, slot_from(i, a), arr)
        p = i + 1
        if tier == 12:
            t = jnp.where(p < 3, p - 1, 2 * p - 4)
        else:
            t = 2 * p - (16 - tier)
        give_back(t)

        @pl.when(p >= (3 if tier == 12 else 0))
        def _():
            give_back(t + 1)

        return carry

    lax.fori_loop(1, FAR, step, 0)

    for i in range(FAR, FAR + 2):
        at = jnp.int32(i)
        for d in range(2):
            ring_copy(at, d, i).wait_recv()
            core_copy(at, d, i).start()
        for d in range(2):
            core_copy(at, d, i).wait_recv()
        solve(8 + i, slot_from(at, 0), arr)
        give_back(first_position(tier, 8 + i))

    def drain(i, carry):
        for d in range(2):
            ring_copy(i, d).wait_send()
            core_copy(i, d).wait_send()
        return carry

    lax.fori_loop(0, FAR, drain, 0)
    for i in range(FAR, FAR + 2):
        for d in range(2):
            ring_copy(jnp.int32(i), d, i).wait_send()
            core_copy(jnp.int32(i), d, i).wait_send()

    def drain_out(p, carry):
        wait_bytes(arr, p, PLANE - 1, out_ss.at[p])
        return carry

    lax.fori_loop(0, tier // 2, drain_out, 0)

    def drain_back(t, carry):
        wait_bytes(back, t, PLANE - 1, ret_ss.at[t])
        wait_bytes(back, t, PLANE, ret_rs.at[t])
        return carry

    lax.fori_loop(0, tier, drain_back, 0)


def exchange(tier, table, pattern, rhs, pinv, ufac):
    vmem = pl.BlockSpec(memory_space=pltpu.VMEM)
    hbm = pl.BlockSpec(memory_space=pl.ANY)
    dma = pltpu.SemaphoreType.DMA
    f32 = jnp.float32
    return pl.pallas_call(
        functools.partial(exchange_kernel, tier),
        out_shape=(
            jax.ShapeDtypeStruct((RING_SLOTS, PLANE * MSG, BLOCK), f32),
            jax.ShapeDtypeStruct((ROW_BLOCKS * 8, BLOCK), f32),
        ),
        in_specs=[hbm] * 5,
        out_specs=(hbm, vmem),
        scratch_shapes=[
            pltpu.SMEM(table.shape, jnp.int32),
            pltpu.VMEM(pattern.shape, jnp.int32),
            pltpu.VMEM(rhs.shape, f32),
            pltpu.VMEM(pinv.shape, f32),
            pltpu.VMEM(ufac.shape, f32),
            pltpu.VMEM((ROW_BLOCKS, BLOCK), f32),
            pltpu.VMEM((PAIRS, PLANE, MSG, BLOCK), f32),
            pltpu.VMEM((RING_SLOTS, PACKED, BLOCK), f32),
            pltpu.VMEM((NEAR, PLANE * MSG, BLOCK), f32),
            pltpu.VMEM((PAIRS, PLANE * MSG, BLOCK), f32),
            pltpu.VMEM((RING_SLOTS, PLANE * MSG, BLOCK), f32),
            pltpu.VMEM((RING_SLOTS, PLANE * MSG, BLOCK), f32),
            dma((5,)),
            dma((2, FAR + 2)), dma((2, FAR + 2)), dma((2, FAR + 2)), dma((2, FAR + 2)),
            dma((PAIRS,)), dma((PAIRS,)), dma((RING_SLOTS,)), dma((RING_SLOTS,)),
        ],
        compiler_params=pltpu.CompilerParams(
            collective_id=TIERS.index(tier), has_side_effects=True, vmem_limit_bytes=36 * 1024 * 1024
        ),
        name=f"exchange_{tier}",
    )(table, pattern, rhs, pinv, ufac)


def assemble_kernel(table, slots, blocks, ret, acc_in, out, acc, sems):
    z = lax.rem(lax.div(lax.axis_index("rows"), NX), NZ)
    acc[...] = acc_in[...]

    def one_front(f, carry):
        o, ring = sequence_of(slots[f], z)
        at = ((table[o, z * PLANE + ring] >> 8) & 255) * PLANE + ring
        for h in range(4):
            rows = pl.ds(pl.multiple_of(blocks[h, f] * 8, 8), COLS)
            v = ret[at, pl.ds(h, COLS, stride=4), :]
            acc[rows, :] = v if h < 2 else acc[rows, :] - v
        return carry

    lax.fori_loop(0, slots.shape[0], one_front, 0, unroll=4)

    def regroup(k, carry):
        for j in range(COLS):
            rows = pl.ds(pl.multiple_of(j * ROW_BLOCKS + 8 * k, 8), 8)
            out[rows, :] = acc[pl.ds(64 * k + j, 8, stride=8), :]
        return carry

    lax.fori_loop(0, ROW_BLOCKS // 8, regroup, 0, unroll=2)


def assemble(table, slots, blocks, ret, acc):
    vmem = pl.BlockSpec(memory_space=pltpu.VMEM)
    smem = pl.BlockSpec(memory_space=pltpu.SMEM)
    return pl.pallas_call(
        assemble_kernel,
        out_shape=jax.ShapeDtypeStruct((COLS * ROW_BLOCKS, BLOCK), jnp.float32),
        in_specs=[smem, smem, smem, vmem, vmem],
        out_specs=vmem,
        scratch_shapes=[pltpu.VMEM(acc.shape, jnp.float32), pltpu.SemaphoreType.DMA],
        compiler_params=pltpu.CompilerParams(vmem_limit_bytes=16 * 1024 * 1024),
        name="assemble",
    )(table, slots, blocks, ret, acc)


def branch(tier, table, slots, blocks, pattern, rhs, pinv, ufac):
    ret, acc = exchange(tier, table, pattern, rhs, pinv, ufac)
    return assemble(table, slots, blocks, ret.reshape(RING_SLOTS * PLANE, MSG, BLOCK), acc)


def on_device(rhs, pattern, front_blocks, front_slot, pivot_inverse, update_factor):
    shape = rhs.shape
    blocks = front_blocks.T
    table, tier = make_tables(front_slot, blocks)
    out = lax.switch(
        tier[0],
        [functools.partial(branch, t) for t in TIERS],
        table, front_slot, blocks, pattern.T, rhs.reshape(COLS * ROW_BLOCKS, BLOCK), pivot_inverse, update_factor,
    )
    return out.reshape(shape)


def solution(mesh):
    return jax.shard_map(
        on_device,
        mesh=mesh,
        in_specs=(
            P("cols", "rows", None),
            P(None, "cols"),
            P(),
            P(),
            P("rows", None, None),
            P("rows", None, None),
        ),
        out_specs=P("cols", "rows", None),
        check_vma=False,
    )
```

```python
import functools

import jax
import jax.numpy as jnp
from jax import lax
from jax.experimental import pallas as pl
from jax.experimental.pallas import tpu as pltpu
from jax.sharding import PartitionSpec as P

BLOCK = 128
PIV = 256
NX, NY, NZ = 4, 4, 8
PLANE = NX * NY
SLOT_DEV = 2
PAIRS = NZ
RING_SLOTS = NZ * SLOT_DEV
COLS = 6
ROW_BLOCKS = 384
MSG = COLS * 4
FAR = 6
PACKED = 768
MESH = pl.DeviceIdType.MESH
PEERS = (
    (2, 2), (2, 1), (2, 3), (1, 2), (3, 2), (1, 1), (3, 3), (1, 3),
    (3, 1), (0, 2), (2, 0), (0, 1), (1, 0), (0, 3), (3, 0),
)


def nt(a, b):
    return lax.dot_general(a, b, (((1,), (1,)), ((), ())), preferred_element_type=jnp.float32)


def nn(a, b):
    return lax.dot_general(a, b, (((1,), (0,)), ((), ())), preferred_element_type=jnp.float32)


def split(v):
    high = v.astype(jnp.bfloat16)
    low = (v - high.astype(jnp.float32)).astype(jnp.bfloat16)
    return high, low


def product(dot, x, w):
    xh, xl = split(x)
    wh, wl = split(w)
    both = dot(jnp.concatenate([xh, xl], axis=0), wh)
    n = x.shape[0]
    return both[:n] + (both[n:] + dot(xh, wl))


TIERS = (12, 14, 16)


def first_position(tier, o):
    p = o // 2
    last = o - 14 if p == PAIRS - 1 else 0
    if tier == 12:
        return (max(p - 1, 0) if p < 3 else 2 * p - 4) + last
    return max(2 * p - (16 - tier), 0) + last


def slot_in_sequence(o, z, ring):
    p, a = o >> 1, o & 1
    i = p - 1
    reach = (i >> 1) + 1
    edge = jnp.logical_or(p == 0, p == PAIRS - 1)
    zs = jnp.where(p == 0, z, jnp.where(a == 0, z - reach, z + reach)) & (NZ - 1)
    sl = jnp.where(edge, a, i & 1)
    zs = jnp.where(p == PAIRS - 1, z + NZ // 2, zs) & (NZ - 1)
    return (((ring >> 2) * NZ + zs) * NX + (ring & (NX - 1))) * SLOT_DEV + sl


def sequence_of(slot, z):
    sl = slot & 1
    ring = ((slot >> 6) << 2) + ((slot >> 1) & 3)
    delta = (z - (slot >> 3)) & (NZ - 1)
    below = delta < NZ // 2
    o = 4 * jnp.where(below, delta, NZ - delta) - 2 + 2 * sl + jnp.where(below, 0, 1)
    o = jnp.where(delta == NZ // 2, 2 * (PAIRS - 1) + sl, o)
    return jnp.where(delta == 0, sl, o), ring


def tables_kernel(slots_h, blocks_h, pinv_h, ufac_h, table, own, tier_ref, slots, blocks, pinv, ufac, sems):
    fetches = [
        pltpu.make_async_copy(src, dst, sems.at[k])
        for k, (src, dst) in enumerate(((slots_h, slots), (blocks_h, blocks), (pinv_h, pinv), (ufac_h, ufac)))
    ]
    for fetch in fetches:
        fetch.start()
    shape = (RING_SLOTS, 128)
    o_of = lax.broadcasted_iota(jnp.int32, shape, 0)
    lane = lax.broadcasted_iota(jnp.int32, shape, 1)
    slot_of = slot_in_sequence(o_of, lane >> 4, lane & 15)
    fetches[0].wait()
    fetches[1].wait()

    def mark(f, code):
        for k in range(8):
            g = 8 * f + k
            code = jnp.where(slot_of == slots[g], 1 + blocks[0, g] + (blocks[1, g] << 9), code)
        return code

    code = lax.fori_loop(0, slots.shape[0] // 8, mark, jnp.zeros(shape, jnp.int32))
    used = code > 0
    count = jnp.zeros((1, 128), jnp.int32)
    ranks = []
    last = {t: jnp.full((1, 128), -1, jnp.int32) for t in TIERS}
    places = {t: [] for t in TIERS}
    for o in range(RING_SLOTS):
        on = used[o : o + 1]
        ranks.append(jnp.where(on, count, 0))
        count = count + on.astype(jnp.int32)
        for t in TIERS:
            last[t] = jnp.where(on, jnp.maximum(last[t] + 1, first_position(t, o)), last[t])
            places[t].append(jnp.where(on, last[t], 255))
    fits = [jnp.max(last[t]) < t for t in TIERS]
    tier = jnp.where(fits[0], 0, jnp.where(fits[1], 1, 2))
    place = {t: jnp.concatenate(places[t], axis=0) for t in TIERS}
    place = jnp.where(tier == 0, place[TIERS[0]], jnp.where(tier == 1, place[TIERS[1]], place[TIERS[2]]))
    holds = jnp.zeros(shape, jnp.int32)
    by_rank = jnp.zeros(shape, jnp.int32)
    for o in range(RING_SLOTS):
        holds = jnp.where(place[o : o + 1] == o_of, o, holds)
        mine = jnp.logical_and(used[o : o + 1], ranks[o] == o_of)
        by_rank = jnp.where(mine, code[o : o + 1] - 1, by_rank)
    table[0:RING_SLOTS, :] = jnp.concatenate(ranks, axis=0) + (place << 8) + (holds << 16)
    table[RING_SLOTS : 2 * RING_SLOTS, :] = by_rank
    tier_ref[0] = tier
    fetches[2].wait()
    fetches[3].wait()

    row = lax.broadcasted_iota(jnp.int32, (BLOCK, BLOCK), 0)
    col = lax.broadcasted_iota(jnp.int32, (BLOCK, BLOCK), 1)
    for s in range(SLOT_DEV):
        own[s, 0:BLOCK, :] = jnp.where(
            row > col, pinv[s, :BLOCK, :BLOCK], pinv[s, BLOCK:, BLOCK:].T
        )
        own[s, BLOCK : 2 * BLOCK, :] = pinv[s, BLOCK:, :BLOCK]
        own[s, PIV : 2 * PIV, :] = ufac[s, :, :BLOCK]
        own[s, 2 * PIV : 3 * PIV, :] = ufac[s, :, BLOCK:]


def make_tables(slots, blocks, pinv, ufac):
    hbm = pl.BlockSpec(memory_space=pltpu.HBM)
    vmem = pl.BlockSpec(memory_space=pltpu.VMEM)
    return pl.pallas_call(
        tables_kernel,
        out_shape=(
            jax.ShapeDtypeStruct((2 * RING_SLOTS, 128), jnp.int32),
            jax.ShapeDtypeStruct((SLOT_DEV, PACKED, BLOCK), jnp.float32),
            jax.ShapeDtypeStruct((1,), jnp.int32),
        ),
        in_specs=[hbm] * 4,
        out_specs=(vmem, vmem, pl.BlockSpec(memory_space=pltpu.SMEM)),
        scratch_shapes=[
            pltpu.SMEM(slots.shape, jnp.int32),
            pltpu.SMEM(blocks.shape, jnp.int32),
            pltpu.VMEM(pinv.shape, jnp.float32),
            pltpu.VMEM(ufac.shape, jnp.float32),
            pltpu.SemaphoreType.DMA((4,)),
        ],
        compiler_params=pltpu.CompilerParams(vmem_limit_bytes=66_200_000),
        name="tables",
    )(slots, blocks, pinv, ufac)


def exchange_kernel(
    tier, own, table_h, slots_h, pattern_h, rhs_h, ret, acc, where,
    table, slots, pattern, rhs, mask, send, fac, land, arr, res, back, in_sems,
    ring_ss, ring_rs, core_ss, core_rs, out_ss, out_rs, ret_ss, ret_rs,
):
    r = lax.axis_index("rows")
    c = lax.axis_index("cols")
    x = lax.rem(r, NX)
    z = lax.rem(lax.div(r, NX), NZ)
    y = lax.div(r, NX * NZ)
    me = y * NX + x

    def chip(yy, zz, xx):
        return (yy * NZ + zz) * NX + xx

    def peer(dy, dx):
        return lax.rem(y + dy, NY), lax.rem(x + dx, NX)

    above = lax.rem(z + 1, NZ)
    below = lax.rem(z + NZ - 1, NZ)

    barrier = pltpu.get_barrier_semaphore()
    for dy, dx in PEERS:
        py, px = peer(dy, dx)
        pl.semaphore_signal(barrier, inc=1, device_id=(chip(py, z, px), c), device_id_type=MESH)
    for zz in (above, below):
        pl.semaphore_signal(barrier, inc=1, device_id=(chip(y, zz, x), c), device_id_type=MESH)
    pl.semaphore_signal(barrier, inc=1, device_id=(r, 1 - c), device_id_type=MESH)

    fetches = [
        pltpu.make_async_copy(src, dst, in_sems.at[k])
        for k, (src, dst) in enumerate(
            ((table_h, table), (pattern_h, pattern), (rhs_h, rhs), (slots_h, slots))
        )
    ]
    for fetch in fetches:
        fetch.start()
    pl.semaphore_wait(barrier, len(PEERS) + 3)

    def slot_at(i, d, away):
        zs = lax.rem(z - (1 - 2 * d) * (lax.div(i, 2) + away) + NZ, NZ)
        return SLOT_DEV * zs + lax.rem(i, 2)

    def slot_from(i, d):
        return slot_at(i, d, 1)

    def piece(k):
        at = (2 * c + k) * (PACKED // 4)
        return pl.ds(pl.multiple_of(at, PACKED // 4), PACKED // 4)

    def ring_copy(i, d, k, source=None):
        view = fac.at[slot_at(i, d, 0), piece(k), :]
        source = view if source is None else source.at[piece(k), :]
        return pltpu.make_async_remote_copy(
            source, view, ring_ss.at[d, k, i], ring_rs.at[d, k, i],
            device_id=(chip(y, (above, below)[d], x), c), device_id_type=MESH,
        )

    def core_copy(i, d, k):
        view = fac.at[slot_from(i, d), piece(k), :]
        return pltpu.make_async_remote_copy(
            view, view, core_ss.at[d, k, i], core_rs.at[d, k, i],
            device_id=(r, 1 - c), device_id_type=MESH,
        )

    pieces = tuple((k, d) for k in range(2) for d in range(2))
    far_pieces = ((0, 0), (1, 1))

    lane = z * PLANE + me

    def pack(p):
        def one(m, carry):
            for a in range(2):
                code = table[RING_SLOTS + 2 * p + a, z * PLANE + m]
                for h, b in enumerate((code & 511, code >> 9)):
                    v = rhs[pl.ds(b, COLS, stride=ROW_BLOCKS), :] * mask[pl.ds(b, 1), :]
                    send[p, m, pl.ds(2 * a + h, COLS, stride=4), :] = v
            return carry

        lax.fori_loop(0, PLANE, one, 0, unroll=2)

    def rows_at(ref, p, m):
        return ref.at[p, pl.ds(pl.multiple_of(m * MSG, 8), MSG), :]

    def start_out(p):
        for dy, dx in PEERS:
            py, px = peer(dy, dx)
            pltpu.make_async_remote_copy(
                send.at[p, py * NX + px], rows_at(land, p, me), out_ss.at[p], out_rs.at[p],
                device_id=(chip(py, z, px), c), device_id_type=MESH,
            ).start()
        land[p, pl.ds(pl.multiple_of(me * MSG, 8), MSG), :] = send[p, me]

    def start_back(t):
        for dy, dx in PEERS:
            py, px = peer(dy, dx)
            pltpu.make_async_remote_copy(
                rows_at(back, t, py * NX + px), rows_at(ret, t, me), ret_ss.at[t], ret_rs.at[t],
                device_id=(chip(py, z, px), c), device_id_type=MESH,
            ).start()
        pltpu.make_async_copy(rows_at(back, t, me), rows_at(ret, t, me), ret_rs.at[t]).start()

    def wait_bytes(ref, p, n, sem):
        view = ref.at[p, pl.ds(0, n * MSG), :]
        pltpu.make_async_copy(view, view, sem).wait()

    row = lax.broadcasted_iota(jnp.int32, (BLOCK, BLOCK), 0)
    col = lax.broadcasted_iota(jnp.int32, (BLOCK, BLOCK), 1)

    def solve(o, factor):
        k = table[o, lane] & 255
        data = arr.at[k >> 1]
        second = (k & 1) == 1
        x0, x1 = (
            jnp.where(
                second,
                data[pl.ds(2 + h, PLANE * COLS, stride=4), :],
                data[pl.ds(h, PLANE * COLS, stride=4), :],
            )
            for h in range(2)
        )
        merged = factor[0:BLOCK, :]
        lower = jnp.where(row > col, merged, 0.0)
        upper = jnp.where(row < col, merged, 0.0)
        left = jnp.concatenate([lower, factor[BLOCK:PIV, :]], axis=0)
        first = product(nt, x0, left)
        y0 = x0 + first[:, :BLOCK]
        y1 = x1 + (first[:, BLOCK:] + product(nn, x1, upper))
        upd = product(nt, y0, factor[PIV : 2 * PIV, :]) + product(nt, y1, factor[2 * PIV : 3 * PIV, :])
        for h, v in enumerate((y0, y1, upd[:, :BLOCK], upd[:, BLOCK:])):
            res[o, pl.ds(h, PLANE * COLS, stride=4), :] = v

    def give_back(t):
        back[t] = res[table[t, lane] >> 16]
        start_back(t)

    for i in range(SLOT_DEV):
        for k, d in pieces:
            ring_copy(jnp.int32(i), d, k, own.at[i]).start()
    fetches[1].wait()
    for k in range(ROW_BLOCKS // BLOCK):
        on = pattern[:, k * BLOCK : (k + 1) * BLOCK].astype(jnp.float32)
        mask[k * BLOCK : (k + 1) * BLOCK, :] = jnp.broadcast_to(on, (BLOCK, BLOCK)).T
    fetches[0].wait()
    fetches[2].wait()

    def out_step(p, carry):
        pack(p)
        start_out(p)
        return carry

    lax.fori_loop(0, tier // 2, out_step, 0)

    def init(k, carry):
        on = mask[pl.ds(pl.multiple_of(8 * k, 8), 8), :]
        for j in range(COLS):
            v = rhs[pl.ds(pl.multiple_of(j * ROW_BLOCKS + 8 * k, 8), 8), :] * on
            acc[pl.ds(64 * k + j, 8, stride=8), :] = v
        return carry

    lax.fori_loop(0, ROW_BLOCKS // 8, init, 0, unroll=2)
    fetches[3].wait()

    def locate(f, carry):
        o, ring = sequence_of(slots[f], z)
        where[f] = ((table[o, z * PLANE + ring] >> 8) & 255) * PLANE + ring
        return carry

    lax.fori_loop(0, slots.shape[0], locate, 0, unroll=8)

    def forward(i):
        for k, d in pieces:
            ring_copy(i, d, k).wait_recv()

            @pl.when(i < (FAR if k == d else FAR - 2))
            def _():
                ring_copy(i + 2, d, k).start()

            core_copy(i, d, k).start()

    def collect(i):
        for k, d in pieces:
            core_copy(i, d, k).wait_recv()

    def arrive(p):
        wait_bytes(land, p, PLANE - 1, out_rs.at[p])
        arr[p] = land[p]

    zero = jnp.int32(0)
    forward(zero)
    arrive(0)
    for a in range(2):
        solve(a, own.at[a])
    for t in range(first_position(tier, 2)):
        give_back(t)
    arrive(1)
    collect(zero)
    for a in range(2):
        solve(2 + a, fac.at[slot_from(zero, a)])
    for t in range(first_position(tier, 2), first_position(tier, 4)):
        give_back(t)

    def step(i, carry):
        forward(i)

        @pl.when(i + 1 < tier // 2)
        def _():
            arrive(i + 1)

        collect(i)
        for a in range(2):
            solve(2 * i + 2 + a, fac.at[slot_from(i, a)])
        p = i + 1
        if tier == 12:
            t = jnp.where(p < 3, p - 1, 2 * p - 4)
        else:
            t = 2 * p - (16 - tier)
        give_back(t)

        @pl.when(p >= (3 if tier == 12 else 0))
        def _():
            give_back(t + 1)

        return carry

    lax.fori_loop(1, FAR, step, 0)

    if tier == 2 * PAIRS:
        arrive(PAIRS - 1)
    for i in range(FAR, FAR + 2):
        at = jnp.int32(i)
        for k, d in far_pieces:
            ring_copy(at, d, k).wait_recv()
            core_copy(at, d, k).start()
        for k, d in far_pieces:
            core_copy(at, d, k).wait_recv()
        solve(8 + i, fac.at[slot_from(at, 0)])
        give_back(first_position(tier, 8 + i))

    def drain(i, carry):
        for k, d in pieces:
            ring_copy(i, d, k).wait_send()
            core_copy(i, d, k).wait_send()
        return carry

    lax.fori_loop(0, FAR, drain, 0)
    for i in range(FAR, FAR + 2):
        for k, d in far_pieces:
            ring_copy(jnp.int32(i), d, k).wait_send()
            core_copy(jnp.int32(i), d, k).wait_send()

    def drain_out(p, carry):
        wait_bytes(arr, p, PLANE - 1, out_ss.at[p])
        return carry

    lax.fori_loop(0, tier // 2, drain_out, 0)

    def drain_back(t, carry):
        wait_bytes(back, t, PLANE - 1, ret_ss.at[t])
        wait_bytes(back, t, PLANE, ret_rs.at[t])
        return carry

    lax.fori_loop(0, tier, drain_back, 0)


def exchange(tier, own, table, slots, pattern, rhs):
    vmem = pl.BlockSpec(memory_space=pltpu.VMEM)
    hbm = pl.BlockSpec(memory_space=pl.ANY)
    dma = pltpu.SemaphoreType.DMA
    f32 = jnp.float32
    return pl.pallas_call(
        functools.partial(exchange_kernel, tier),
        out_shape=(
            jax.ShapeDtypeStruct((RING_SLOTS, PLANE * MSG, BLOCK), f32),
            jax.ShapeDtypeStruct((ROW_BLOCKS * 8, BLOCK), f32),
            jax.ShapeDtypeStruct(slots.shape, jnp.int32),
        ),
        in_specs=[vmem] + [hbm] * 4,
        out_specs=(hbm, vmem, pl.BlockSpec(memory_space=pltpu.SMEM)),
        scratch_shapes=[
            pltpu.SMEM(table.shape, jnp.int32),
            pltpu.SMEM(slots.shape, jnp.int32),
            pltpu.VMEM(pattern.shape, jnp.int32),
            pltpu.VMEM(rhs.shape, f32),
            pltpu.VMEM((ROW_BLOCKS, BLOCK), f32),
            pltpu.VMEM((PAIRS, PLANE, MSG, BLOCK), f32),
            pltpu.VMEM((RING_SLOTS, PACKED, BLOCK), f32),
            pltpu.VMEM((PAIRS, PLANE * MSG, BLOCK), f32),
            pltpu.VMEM((PAIRS, PLANE * MSG, BLOCK), f32),
            pltpu.VMEM((RING_SLOTS, PLANE * MSG, BLOCK), f32),
            pltpu.VMEM((RING_SLOTS, PLANE * MSG, BLOCK), f32),
            dma((4,)),
            *[dma((2, 2, FAR + 2))] * 4,
            dma((PAIRS,)), dma((PAIRS,)), dma((RING_SLOTS,)), dma((RING_SLOTS,)),
        ],
        compiler_params=pltpu.CompilerParams(
            collective_id=TIERS.index(tier), has_side_effects=True, vmem_limit_bytes=36 * 1024 * 1024
        ),
        name=f"exchange_{tier}",
    )(own, table, slots, pattern, rhs)


def assemble_kernel(where, blocks, ret, acc_in, out_h, acc, out, sems):
    del acc_in

    def one_front(f, carry):
        at = where[f]
        for h in range(4):
            rows = pl.ds(pl.multiple_of(blocks[h, f] * 8, 8), COLS)
            v = ret[at, pl.ds(h, COLS, stride=4), :]
            acc[rows, :] = v if h < 2 else acc[rows, :] - v
        return carry

    lax.fori_loop(0, where.shape[0], one_front, 0, unroll=8)

    copies = []
    for j in range(COLS):

        def regroup(k, carry):
            rows = pl.ds(pl.multiple_of(j * ROW_BLOCKS + 8 * k, 8), 8)
            out[rows, :] = acc[pl.ds(64 * k + j, 8, stride=8), :]
            return carry

        lax.fori_loop(0, ROW_BLOCKS // 8, regroup, 0, unroll=8)
        rows = pl.ds(j * ROW_BLOCKS, ROW_BLOCKS)
        copies.append(pltpu.make_async_copy(out.at[rows, :], out_h.at[rows, :], sems.at[j]))
        copies[-1].start()
    for copy in copies:
        copy.wait()


def assemble(where, blocks, ret, acc):
    vmem = pl.BlockSpec(memory_space=pltpu.VMEM)
    smem = pl.BlockSpec(memory_space=pltpu.SMEM)
    shape = (COLS * ROW_BLOCKS, BLOCK)
    return pl.pallas_call(
        assemble_kernel,
        out_shape=(
            jax.ShapeDtypeStruct(shape, jnp.float32),
            jax.ShapeDtypeStruct(acc.shape, jnp.float32),
        ),
        in_specs=[smem, smem, vmem, vmem],
        out_specs=(pl.BlockSpec(memory_space=pltpu.HBM), vmem),
        scratch_shapes=[pltpu.VMEM(shape, jnp.float32), pltpu.SemaphoreType.DMA((COLS,))],
        input_output_aliases={3: 1},
        compiler_params=pltpu.CompilerParams(vmem_limit_bytes=16 * 1024 * 1024),
        name="assemble",
    )(where, blocks, ret, acc)[0]


def branch(tier, own, table, slots, blocks, pattern, rhs):
    ret, acc, where = exchange(tier, own, table, slots, pattern, rhs)
    return assemble(where, blocks, ret.reshape(RING_SLOTS * PLANE, MSG, BLOCK), acc)


def on_device(rhs, pattern, front_blocks, front_slot, pivot_inverse, update_factor):
    shape = rhs.shape
    blocks = front_blocks.T
    table, own, tier = make_tables(front_slot, blocks, pivot_inverse, update_factor)
    out = lax.switch(
        tier[0],
        [functools.partial(branch, t) for t in TIERS],
        own, table, front_slot, blocks, pattern.T, rhs.reshape(COLS * ROW_BLOCKS, BLOCK),
    )
    return out.reshape(shape)


def solution(mesh):
    return jax.shard_map(
        on_device,
        mesh=mesh,
        in_specs=(
            P("cols", "rows", None),
            P(None, "cols"),
            P(),
            P(),
            P("rows", None, None),
            P("rows", None, None),
        ),
        out_specs=P("cols", "rows", None),
        check_vma=False,
    )
```

```python
import functools

import jax
import jax.numpy as jnp
from jax import lax
from jax.experimental import pallas as pl
from jax.experimental.pallas import tpu as pltpu
from jax.sharding import PartitionSpec as P

BLOCK = 128
PIV = 256
NX, NY, NZ = 4, 4, 8
PLANE = NX * NY
SLOT_DEV = 2
PAIRS = NZ
RING_SLOTS = NZ * SLOT_DEV
COLS = 6
ROW_BLOCKS = 384
MSG = COLS * 4
FAR = 6
PACKED = 768
MESH = pl.DeviceIdType.MESH
PEERS = (
    (2, 2), (2, 1), (2, 3), (1, 2), (3, 2), (1, 1), (3, 3), (1, 3),
    (3, 1), (0, 2), (2, 0), (0, 1), (1, 0), (0, 3), (3, 0),
)


def nt(a, b):
    return lax.dot_general(a, b, (((1,), (1,)), ((), ())), preferred_element_type=jnp.float32)


def nn(a, b):
    return lax.dot_general(a, b, (((1,), (0,)), ((), ())), preferred_element_type=jnp.float32)


def split(v):
    high = v.astype(jnp.bfloat16)
    low = (v - high.astype(jnp.float32)).astype(jnp.bfloat16)
    return high, low


def product(dot, x, w):
    xh, xl = split(x)
    wh, wl = split(w)
    both = dot(jnp.concatenate([xh, xl], axis=0), wh)
    n = x.shape[0]
    return both[:n] + (both[n:] + dot(xh, wl))


TIERS = (12, 14, 16)


def first_position(tier, o):
    p, a = o // 2, o % 2
    if tier == 12:
        return max(p - 1, 0) if p < 3 else 2 * p - 4 + a
    return max(2 * p - (16 - tier) + a, 0) if p else a * (tier == 16)


def slot_in_sequence(o, z, ring):
    p, a = o >> 1, o & 1
    i = p - 1
    reach = (i >> 1) + 1
    edge = jnp.logical_or(p == 0, p == PAIRS - 1)
    lower = (a ^ jnp.where(z < NZ // 2, 1, 0)) == 0
    zs = jnp.where(p == 0, z, jnp.where(lower, z - reach, z + reach)) & (NZ - 1)
    sl = jnp.where(edge, a, i & 1)
    zs = jnp.where(p == PAIRS - 1, z + NZ // 2, zs) & (NZ - 1)
    return (((ring >> 2) * NZ + zs) * NX + (ring & (NX - 1))) * SLOT_DEV + sl


def sequence_of(slot, z):
    sl = slot & 1
    ring = ((slot >> 6) << 2) + ((slot >> 1) & 3)
    delta = (z - (slot >> 3)) & (NZ - 1)
    below = delta < NZ // 2
    o = 4 * jnp.where(below, delta, NZ - delta) - 2 + 2 * sl
    o = o + (jnp.where(below, 0, 1) ^ jnp.where(z < NZ // 2, 1, 0))
    o = jnp.where(delta == NZ // 2, 2 * (PAIRS - 1) + sl, o)
    return jnp.where(delta == 0, sl, o), ring


def tables_kernel(slots_h, pinv_h, ufac_h, table, own, tier_ref, slots, pinv, ufac, sems):
    fetches = [
        pltpu.make_async_copy(src, dst, sems.at[k])
        for k, (src, dst) in enumerate(((slots_h, slots), (pinv_h, pinv), (ufac_h, ufac)))
    ]
    for fetch in fetches:
        fetch.start()
    shape = (RING_SLOTS, 128)
    o_of = lax.broadcasted_iota(jnp.int32, shape, 0)
    lane = lax.broadcasted_iota(jnp.int32, shape, 1)
    slot_of = slot_in_sequence(o_of, lane >> 4, lane & 15)
    fetches[0].wait()

    def mark(f, code):
        for k in range(16):
            g = 16 * f + k
            code = jnp.where(slot_of == slots[g], 1 + g, code)
        return code

    code = lax.fori_loop(0, slots.shape[0] // 16, mark, jnp.zeros(shape, jnp.int32))
    used = code > 0
    count = jnp.zeros((1, 128), jnp.int32)
    ranks = []
    last = {t: jnp.full((1, 128), -1, jnp.int32) for t in TIERS}
    places = {t: [] for t in TIERS}
    for o in range(RING_SLOTS):
        on = used[o : o + 1]
        ranks.append(jnp.where(on, count, 0))
        count = count + on.astype(jnp.int32)
        for t in TIERS:
            last[t] = jnp.where(on, jnp.maximum(last[t] + 1, first_position(t, o)), last[t])
            places[t].append(jnp.where(on, last[t], 255))
    fits = [jnp.max(last[t]) < t for t in TIERS]
    tier = jnp.where(fits[0], 0, jnp.where(fits[1], 1, 2))
    place = {t: jnp.concatenate(places[t], axis=0) for t in TIERS}
    place = jnp.where(tier == 0, place[TIERS[0]], jnp.where(tier == 1, place[TIERS[1]], place[TIERS[2]]))
    holds = jnp.zeros(shape, jnp.int32)
    by_rank = jnp.zeros(shape, jnp.int32)
    for o in range(RING_SLOTS):
        holds = jnp.where(place[o : o + 1] == o_of, o, holds)
        mine = jnp.logical_and(used[o : o + 1], ranks[o] == o_of)
        by_rank = jnp.where(mine, code[o : o + 1] - 1, by_rank)
    table[0:RING_SLOTS, :] = jnp.concatenate(ranks, axis=0) + (place << 8) + (holds << 16)
    table[RING_SLOTS : 2 * RING_SLOTS, :] = by_rank
    tier_ref[0] = tier
    fetches[1].wait()
    fetches[2].wait()

    row = lax.broadcasted_iota(jnp.int32, (BLOCK, BLOCK), 0)
    col = lax.broadcasted_iota(jnp.int32, (BLOCK, BLOCK), 1)
    for s in range(SLOT_DEV):
        own[s, 0:BLOCK, :] = jnp.where(
            row > col, pinv[s, :BLOCK, :BLOCK], pinv[s, BLOCK:, BLOCK:].T
        )
        own[s, BLOCK : 2 * BLOCK, :] = pinv[s, BLOCK:, :BLOCK]
        own[s, PIV : 2 * PIV, :] = ufac[s, :, :BLOCK]
        own[s, 2 * PIV : 3 * PIV, :] = ufac[s, :, BLOCK:]


def make_tables(slots, pinv, ufac):
    hbm = pl.BlockSpec(memory_space=pltpu.HBM)
    vmem = pl.BlockSpec(memory_space=pltpu.VMEM)
    return pl.pallas_call(
        tables_kernel,
        out_shape=(
            jax.ShapeDtypeStruct((2 * RING_SLOTS, 128), jnp.int32),
            jax.ShapeDtypeStruct((SLOT_DEV, PACKED, BLOCK), jnp.float32),
            jax.ShapeDtypeStruct((1,), jnp.int32),
        ),
        in_specs=[hbm] * 3,
        out_specs=(vmem, vmem, pl.BlockSpec(memory_space=pltpu.SMEM)),
        scratch_shapes=[
            pltpu.SMEM(slots.shape, jnp.int32),
            pltpu.VMEM(pinv.shape, jnp.float32),
            pltpu.VMEM(ufac.shape, jnp.float32),
            pltpu.SemaphoreType.DMA((3,)),
        ],
        compiler_params=pltpu.CompilerParams(vmem_limit_bytes=66_200_000),
        name="tables",
    )(slots, pinv, ufac)


def exchange_kernel(
    tier, own, table_h, slots_h, blocks_h, pattern_h, rhs_h, ret, acc, where,
    table, slots, blocks, pattern, rhs, mask, send, fac, land, arr, res, back, in_sems,
    ring_ss, ring_rs, core_ss, core_rs, out_ss, out_rs, ret_ss, ret_rs,
):
    r = lax.axis_index("rows")
    c = lax.axis_index("cols")
    x = lax.rem(r, NX)
    z = lax.rem(lax.div(r, NX), NZ)
    y = lax.div(r, NX * NZ)
    me = y * NX + x

    def chip(yy, zz, xx):
        return (yy * NZ + zz) * NX + xx

    def peer(dy, dx):
        return lax.rem(y + dy, NY), lax.rem(x + dx, NX)

    above = lax.rem(z + 1, NZ)
    below = lax.rem(z + NZ - 1, NZ)

    barrier = pltpu.get_barrier_semaphore()
    for dy, dx in PEERS:
        py, px = peer(dy, dx)
        pl.semaphore_signal(barrier, inc=1, device_id=(chip(py, z, px), c), device_id_type=MESH)
    for zz in (above, below):
        pl.semaphore_signal(barrier, inc=1, device_id=(chip(y, zz, x), c), device_id_type=MESH)
    pl.semaphore_signal(barrier, inc=1, device_id=(r, 1 - c), device_id_type=MESH)

    fetches = [
        pltpu.make_async_copy(src, dst, in_sems.at[k])
        for k, (src, dst) in enumerate(
            ((table_h, table), (pattern_h, pattern), (rhs_h, rhs), (slots_h, slots), (blocks_h, blocks))
        )
    ]
    for fetch in fetches:
        fetch.start()
    pl.semaphore_wait(barrier, len(PEERS) + 3)

    def slot_at(i, d, away):
        zs = lax.rem(z - (1 - 2 * d) * (lax.div(i, 2) + away) + NZ, NZ)
        return SLOT_DEV * zs + lax.rem(i, 2)

    def slot_from(i, d):
        return slot_at(i, d, 1)

    def piece(k):
        at = (2 * c + k) * (PACKED // 4)
        return pl.ds(pl.multiple_of(at, PACKED // 4), PACKED // 4)

    def ring_copy(i, d, k, source=None):
        view = fac.at[slot_at(i, d, 0), piece(k), :]
        source = view if source is None else source.at[piece(k), :]
        return pltpu.make_async_remote_copy(
            source, view, ring_ss.at[d, k, i], ring_rs.at[d, k, i],
            device_id=(chip(y, jnp.where(d == 0, above, below), x), c), device_id_type=MESH,
        )

    def core_copy(i, d, k):
        view = fac.at[slot_from(i, d), piece(k), :]
        return pltpu.make_async_remote_copy(
            view, view, core_ss.at[d, k, i], core_rs.at[d, k, i],
            device_id=(r, 1 - c), device_id_type=MESH,
        )

    pieces = tuple((k, d) for k in range(2) for d in range(2))
    far_pieces = ((0, 0), (1, 1))

    lane = z * PLANE + me

    def pack(p):
        def one(m, carry):
            for a in range(2):
                f = table[RING_SLOTS + 2 * p + a, z * PLANE + m]
                for h in range(2):
                    b = blocks[h, f]
                    v = rhs[pl.ds(b, COLS, stride=ROW_BLOCKS), :] * mask[pl.ds(b, 1), :]
                    send[p, m, pl.ds(2 * a + h, COLS, stride=4), :] = v
            return carry

        lax.fori_loop(0, PLANE, one, 0, unroll=2)

    def rows_at(ref, p, m):
        return ref.at[p, pl.ds(pl.multiple_of(m * MSG, 8), MSG), :]

    def start_out(p):
        for dy, dx in PEERS:
            py, px = peer(dy, dx)
            pltpu.make_async_remote_copy(
                send.at[p, py * NX + px], rows_at(land, p, me), out_ss.at[p], out_rs.at[p],
                device_id=(chip(py, z, px), c), device_id_type=MESH,
            ).start()
        land[p, pl.ds(pl.multiple_of(me * MSG, 8), MSG), :] = send[p, me]

    def start_back(t):
        for dy, dx in PEERS:
            py, px = peer(dy, dx)
            pltpu.make_async_remote_copy(
                rows_at(back, t, py * NX + px), rows_at(ret, t, me), ret_ss.at[t], ret_rs.at[t],
                device_id=(chip(py, z, px), c), device_id_type=MESH,
            ).start()
        pltpu.make_async_copy(rows_at(back, t, me), rows_at(ret, t, me), ret_rs.at[t]).start()

    def wait_bytes(ref, p, n, sem):
        view = ref.at[p, pl.ds(0, n * MSG), :]
        pltpu.make_async_copy(view, view, sem).wait()

    row = lax.broadcasted_iota(jnp.int32, (BLOCK, BLOCK), 0)
    col = lax.broadcasted_iota(jnp.int32, (BLOCK, BLOCK), 1)

    def solve(o, factor):
        k = table[o, lane] & 255
        data = arr.at[k >> 1]
        second = (k & 1) == 1
        x0, x1 = (
            jnp.where(
                second,
                data[pl.ds(2 + h, PLANE * COLS, stride=4), :],
                data[pl.ds(h, PLANE * COLS, stride=4), :],
            )
            for h in range(2)
        )
        merged = factor[0:BLOCK, :]
        lower = jnp.where(row > col, merged, 0.0)
        upper = jnp.where(row < col, merged, 0.0)
        left = jnp.concatenate([lower, factor[BLOCK:PIV, :]], axis=0)
        first = product(nt, x0, left)
        y0 = x0 + first[:, :BLOCK]
        y1 = x1 + (first[:, BLOCK:] + product(nn, x1, upper))
        upd = product(nt, y0, factor[PIV : 2 * PIV, :]) + product(nt, y1, factor[2 * PIV : 3 * PIV, :])
        for h, v in enumerate((y0, y1, upd[:, :BLOCK], upd[:, BLOCK:])):
            res[o, pl.ds(h, PLANE * COLS, stride=4), :] = v

    def give_back(t):
        back[t] = res[table[t, lane] >> 16]
        start_back(t)

    for i in range(SLOT_DEV):
        for k, d in pieces:
            ring_copy(jnp.int32(i), d, k, own.at[i]).start()
    fetches[1].wait()
    for k in range(ROW_BLOCKS // BLOCK):
        on = pattern[:, k * BLOCK : (k + 1) * BLOCK].astype(jnp.float32)
        mask[k * BLOCK : (k + 1) * BLOCK, :] = jnp.broadcast_to(on, (BLOCK, BLOCK)).T
    fetches[0].wait()
    fetches[4].wait()
    fetches[2].wait()

    def out_step(p, carry):
        pack(p)
        start_out(p)
        return carry

    lax.fori_loop(0, tier // 2, out_step, 0)

    def init(k, carry):
        on = mask[pl.ds(pl.multiple_of(8 * k, 8), 8), :]
        for j in range(COLS):
            v = rhs[pl.ds(pl.multiple_of(j * ROW_BLOCKS + 8 * k, 8), 8), :] * on
            acc[pl.ds(64 * k + j, 8, stride=8), :] = v
        return carry

    lax.fori_loop(0, ROW_BLOCKS // 8, init, 0, unroll=2)
    fetches[3].wait()

    fronts = slots.shape[0]

    def locate(f, carry):
        o, ring = sequence_of(slots[f], z)
        where[f] = (((table[o, z * PLANE + ring] >> 8) & 255) * PLANE + ring) * MSG
        for h in range(4):
            where[(h + 1) * fronts + f] = blocks[h, f] * 8
        return carry

    lax.fori_loop(0, fronts, locate, 0, unroll=4)

    early = jnp.where(z < NZ // 2, 1, 0)

    def forward(i, d):
        for k in range(2):
            ring_copy(i, d, k).wait_recv()

            @pl.when(i < jnp.where(d == k, FAR, FAR - 2))
            def _():
                ring_copy(i + 2, d, k).start()

            core_copy(i, d, k).start()

    def collect(i, d):
        for k in range(2):
            core_copy(i, d, k).wait_recv()

    def arrive(p):
        wait_bytes(land, p, PLANE - 1, out_rs.at[p])
        arr[p] = land[p]

    zero = jnp.int32(0)
    forward(zero, early)
    forward(zero, 1 - early)
    arrive(0)
    for a in range(2):
        solve(a, own.at[a])
    for t in range(first_position(tier, 2)):
        give_back(t)
    arrive(1)
    for a, d in enumerate((early, 1 - early)):
        collect(zero, d)
        solve(2 + a, fac.at[slot_from(zero, d)])
    for t in range(first_position(tier, 2), first_position(tier, 4)):
        give_back(t)

    def step(i, carry):
        p = i + 1
        for a, d in enumerate((early, 1 - early)):
            forward(i, d)
            if a == 0:

                @pl.when(p < tier // 2)
                def _():
                    arrive(p)

            collect(i, d)
            solve(2 * p + a, fac.at[slot_from(i, d)])
            if tier != 12:
                give_back(2 * p - (16 - tier) + a)
            elif a == 0:

                @pl.when(p >= 3)
                def _():
                    give_back(2 * p - 4)

            else:
                give_back(jnp.where(p < 3, p - 1, 2 * p - 3))
        return carry

    lax.fori_loop(1, FAR, step, 0)

    if tier == 2 * PAIRS:
        arrive(PAIRS - 1)
    for i in range(FAR, FAR + 2):
        at = jnp.int32(i)
        for k, d in far_pieces:
            ring_copy(at, d, k).wait_recv()
            core_copy(at, d, k).start()
        for k, d in far_pieces:
            core_copy(at, d, k).wait_recv()
        solve(8 + i, fac.at[slot_from(at, 0)])
        give_back(first_position(tier, 8 + i))

    def drain(i, carry):
        for k, d in pieces:
            ring_copy(i, d, k).wait_send()
            core_copy(i, d, k).wait_send()
        return carry

    lax.fori_loop(0, FAR, drain, 0)
    for i in range(FAR, FAR + 2):
        for k, d in far_pieces:
            ring_copy(jnp.int32(i), d, k).wait_send()
            core_copy(jnp.int32(i), d, k).wait_send()

    def drain_out(p, carry):
        wait_bytes(arr, p, PLANE - 1, out_ss.at[p])
        return carry

    lax.fori_loop(0, tier // 2, drain_out, 0)

    def drain_back(t, carry):
        wait_bytes(back, t, PLANE - 1, ret_ss.at[t])
        wait_bytes(back, t, PLANE, ret_rs.at[t])
        return carry

    lax.fori_loop(0, tier, drain_back, 0)


def exchange(tier, own, table, slots, blocks, pattern, rhs):
    vmem = pl.BlockSpec(memory_space=pltpu.VMEM)
    hbm = pl.BlockSpec(memory_space=pl.ANY)
    dma = pltpu.SemaphoreType.DMA
    f32 = jnp.float32
    return pl.pallas_call(
        functools.partial(exchange_kernel, tier),
        out_shape=(
            jax.ShapeDtypeStruct((RING_SLOTS, PLANE * MSG, BLOCK), f32),
            jax.ShapeDtypeStruct((ROW_BLOCKS * 8, BLOCK), f32),
            jax.ShapeDtypeStruct((5 * slots.shape[0],), jnp.int32),
        ),
        in_specs=[vmem] + [hbm] * 5,
        out_specs=(hbm, vmem, pl.BlockSpec(memory_space=pltpu.SMEM)),
        scratch_shapes=[
            pltpu.SMEM(table.shape, jnp.int32),
            pltpu.SMEM(slots.shape, jnp.int32),
            pltpu.SMEM(blocks.shape, jnp.int32),
            pltpu.VMEM(pattern.shape, jnp.int32),
            pltpu.VMEM(rhs.shape, f32),
            pltpu.VMEM((ROW_BLOCKS, BLOCK), f32),
            pltpu.VMEM((PAIRS, PLANE, MSG, BLOCK), f32),
            pltpu.VMEM((RING_SLOTS, PACKED, BLOCK), f32),
            pltpu.VMEM((PAIRS, PLANE * MSG, BLOCK), f32),
            pltpu.VMEM((PAIRS, PLANE * MSG, BLOCK), f32),
            pltpu.VMEM((RING_SLOTS, PLANE * MSG, BLOCK), f32),
            pltpu.VMEM((RING_SLOTS, PLANE * MSG, BLOCK), f32),
            dma((5,)),
            *[dma((2, 2, FAR + 2))] * 4,
            dma((PAIRS,)), dma((PAIRS,)), dma((RING_SLOTS,)), dma((RING_SLOTS,)),
        ],
        compiler_params=pltpu.CompilerParams(
            collective_id=TIERS.index(tier), has_side_effects=True, vmem_limit_bytes=36 * 1024 * 1024
        ),
        name=f"exchange_{tier}",
    )(own, table, slots, blocks, pattern, rhs)


def assemble_kernel(where, ret, acc_in, out_h, acc, out, sems):
    del acc_in
    fronts = where.shape[0] // 5

    def one_front(f, carry):
        at = pl.multiple_of(where[f], 8)
        for h in range(4):
            rows = pl.ds(pl.multiple_of(where[(h + 1) * fronts + f], 8), COLS)
            v = ret[pl.ds(at + h, COLS, stride=4), :]
            acc[rows, :] = v if h < 2 else acc[rows, :] - v
        return carry

    lax.fori_loop(0, fronts, one_front, 0, unroll=8)

    copies = []
    for j in range(COLS):

        def regroup(k, carry):
            rows = pl.ds(pl.multiple_of(j * ROW_BLOCKS + 8 * k, 8), 8)
            out[rows, :] = acc[pl.ds(64 * k + j, 8, stride=8), :]
            return carry

        lax.fori_loop(0, ROW_BLOCKS // 8, regroup, 0, unroll=8)
        rows = pl.ds(j * ROW_BLOCKS, ROW_BLOCKS)
        copies.append(pltpu.make_async_copy(out.at[rows, :], out_h.at[rows, :], sems.at[j]))
        copies[-1].start()
    for copy in copies:
        copy.wait()


def assemble(where, ret, acc):
    vmem = pl.BlockSpec(memory_space=pltpu.VMEM)
    smem = pl.BlockSpec(memory_space=pltpu.SMEM)
    shape = (COLS * ROW_BLOCKS, BLOCK)
    return pl.pallas_call(
        assemble_kernel,
        out_shape=(
            jax.ShapeDtypeStruct(shape, jnp.float32),
            jax.ShapeDtypeStruct(acc.shape, jnp.float32),
        ),
        in_specs=[smem, vmem, vmem],
        out_specs=(pl.BlockSpec(memory_space=pltpu.HBM), vmem),
        scratch_shapes=[pltpu.VMEM(shape, jnp.float32), pltpu.SemaphoreType.DMA((COLS,))],
        input_output_aliases={2: 1},
        compiler_params=pltpu.CompilerParams(vmem_limit_bytes=16 * 1024 * 1024),
        name="assemble",
    )(where, ret, acc)[0]


def branch(tier, own, table, slots, blocks, pattern, rhs):
    ret, acc, where = exchange(tier, own, table, slots, blocks, pattern, rhs)
    return assemble(where, ret.reshape(RING_SLOTS * PLANE * MSG, BLOCK), acc)


def on_device(rhs, pattern, front_blocks, front_slot, pivot_inverse, update_factor):
    shape = rhs.shape
    blocks = front_blocks.T
    table, own, tier = make_tables(front_slot, pivot_inverse, update_factor)
    out = lax.switch(
        tier[0],
        [functools.partial(branch, t) for t in TIERS],
        own, table, front_slot, blocks, pattern.T, rhs.reshape(COLS * ROW_BLOCKS, BLOCK),
    )
    return out.reshape(shape)


def solution(mesh):
    return jax.shard_map(
        on_device,
        mesh=mesh,
        in_specs=(
            P("cols", "rows", None),
            P(None, "cols"),
            P(),
            P(),
            P("rows", None, None),
            P("rows", None, None),
        ),
        out_specs=P("cols", "rows", None),
        check_vma=False,
    )
```

```python
import functools

import jax
import jax.numpy as jnp
from jax import lax
from jax.experimental import pallas as pl
from jax.experimental.pallas import tpu as pltpu
from jax.sharding import PartitionSpec as P

BLOCK = 128
PIV = 256
NX, NY, NZ = 4, 4, 8
PLANE = NX * NY
SLOT_DEV = 2
PAIRS = NZ
RING_SLOTS = NZ * SLOT_DEV
COLS = 6
ROW_BLOCKS = 384
MSG = COLS * 4
FAR = 6
PACKED = 768
MESH = pl.DeviceIdType.MESH
PEERS = (
    (2, 2), (2, 1), (2, 3), (1, 2), (3, 2), (1, 1), (3, 3), (1, 3),
    (3, 1), (0, 2), (2, 0), (0, 1), (1, 0), (0, 3), (3, 0),
)


def nt(a, b):
    return lax.dot_general(a, b, (((1,), (1,)), ((), ())), preferred_element_type=jnp.float32)


def nn(a, b):
    return lax.dot_general(a, b, (((1,), (0,)), ((), ())), preferred_element_type=jnp.float32)


def split(v):
    high = v.astype(jnp.bfloat16)
    low = (v - high.astype(jnp.float32)).astype(jnp.bfloat16)
    return high, low


def product(dot, x, w):
    xh, xl = split(x)
    wh, wl = split(w)
    both = dot(jnp.concatenate([xh, xl], axis=0), wh)
    n = x.shape[0]
    return both[:n] + (both[n:] + dot(xh, wl))


TIERS = (12, 13, 16)


def pairs_from(tier):
    return max(15 - tier, 0)


def first_position(tier, o):
    p, a = o // 2, o % 2
    start = max(2 * p - (16 - tier), p - 1, 0)
    return start + a if p >= pairs_from(tier) else start


def slot_in_sequence(o, z, ring):
    p, a = o >> 1, o & 1
    i = p - 1
    reach = (i >> 1) + 1
    edge = jnp.logical_or(p == 0, p == PAIRS - 1)
    lower = (a ^ jnp.where(z < NZ // 2, 1, 0)) == 0
    zs = jnp.where(p == 0, z, jnp.where(lower, z - reach, z + reach)) & (NZ - 1)
    sl = jnp.where(edge, a, i & 1)
    zs = jnp.where(p == PAIRS - 1, z + NZ // 2, zs) & (NZ - 1)
    return (((ring >> 2) * NZ + zs) * NX + (ring & (NX - 1))) * SLOT_DEV + sl


def sequence_of(slot, z):
    sl = slot & 1
    ring = ((slot >> 6) << 2) + ((slot >> 1) & 3)
    delta = (z - (slot >> 3)) & (NZ - 1)
    below = delta < NZ // 2
    o = 4 * jnp.where(below, delta, NZ - delta) - 2 + 2 * sl
    o = o + (jnp.where(below, 0, 1) ^ jnp.where(z < NZ // 2, 1, 0))
    o = jnp.where(delta == NZ // 2, 2 * (PAIRS - 1) + sl, o)
    return jnp.where(delta == 0, sl, o), ring


def tables_kernel(slots_h, pinv_h, ufac_h, table, own, tier_ref, slots, pinv, ufac, sems):
    fetches = [
        pltpu.make_async_copy(src, dst, sems.at[k])
        for k, (src, dst) in enumerate(((slots_h, slots), (pinv_h, pinv), (ufac_h, ufac)))
    ]
    for fetch in fetches:
        fetch.start()
    shape = (RING_SLOTS, 128)
    o_of = lax.broadcasted_iota(jnp.int32, shape, 0)
    lane = lax.broadcasted_iota(jnp.int32, shape, 1)
    slot_of = slot_in_sequence(o_of, lane >> 4, lane & 15)
    fetches[0].wait()

    def mark(f, code):
        for k in range(16):
            g = 16 * f + k
            code = jnp.where(slot_of == slots[g], 1 + g, code)
        return code

    code = lax.fori_loop(0, slots.shape[0] // 16, mark, jnp.zeros(shape, jnp.int32))
    used = code > 0
    count = jnp.zeros((1, 128), jnp.int32)
    ranks = []
    last = {t: jnp.full((1, 128), -1, jnp.int32) for t in TIERS}
    places = {t: [] for t in TIERS}
    for o in range(RING_SLOTS):
        on = used[o : o + 1]
        ranks.append(jnp.where(on, count, 0))
        count = count + on.astype(jnp.int32)
        for t in TIERS:
            last[t] = jnp.where(on, jnp.maximum(last[t] + 1, first_position(t, o)), last[t])
            places[t].append(jnp.where(on, last[t], 255))
    fits = [jnp.max(last[t]) < t for t in TIERS]
    tier = jnp.where(fits[0], 0, jnp.where(fits[1], 1, 2))
    place = {t: jnp.concatenate(places[t], axis=0) for t in TIERS}
    place = jnp.where(tier == 0, place[TIERS[0]], jnp.where(tier == 1, place[TIERS[1]], place[TIERS[2]]))
    holds = jnp.zeros(shape, jnp.int32)
    by_rank = jnp.zeros(shape, jnp.int32)
    for o in range(RING_SLOTS):
        holds = jnp.where(place[o : o + 1] == o_of, o, holds)
        mine = jnp.logical_and(used[o : o + 1], ranks[o] == o_of)
        by_rank = jnp.where(mine, code[o : o + 1] - 1, by_rank)
    table[0:RING_SLOTS, :] = jnp.concatenate(ranks, axis=0) + (place << 8) + (holds << 16)
    table[RING_SLOTS : 2 * RING_SLOTS, :] = by_rank
    tier_ref[0] = tier
    fetches[1].wait()
    fetches[2].wait()

    row = lax.broadcasted_iota(jnp.int32, (BLOCK, BLOCK), 0)
    col = lax.broadcasted_iota(jnp.int32, (BLOCK, BLOCK), 1)
    for s in range(SLOT_DEV):
        own[s, 0:BLOCK, :] = jnp.where(
            row > col, pinv[s, :BLOCK, :BLOCK], pinv[s, BLOCK:, BLOCK:].T
        )
        own[s, BLOCK : 2 * BLOCK, :] = pinv[s, BLOCK:, :BLOCK]
        own[s, PIV : 2 * PIV, :] = ufac[s, :, :BLOCK]
        own[s, 2 * PIV : 3 * PIV, :] = ufac[s, :, BLOCK:]


def make_tables(slots, pinv, ufac):
    hbm = pl.BlockSpec(memory_space=pltpu.HBM)
    vmem = pl.BlockSpec(memory_space=pltpu.VMEM)
    return pl.pallas_call(
        tables_kernel,
        out_shape=(
            jax.ShapeDtypeStruct((2 * RING_SLOTS, 128), jnp.int32),
            jax.ShapeDtypeStruct((SLOT_DEV, PACKED, BLOCK), jnp.float32),
            jax.ShapeDtypeStruct((1,), jnp.int32),
        ),
        in_specs=[hbm] * 3,
        out_specs=(vmem, vmem, pl.BlockSpec(memory_space=pltpu.SMEM)),
        scratch_shapes=[
            pltpu.SMEM(slots.shape, jnp.int32),
            pltpu.VMEM(pinv.shape, jnp.float32),
            pltpu.VMEM(ufac.shape, jnp.float32),
            pltpu.SemaphoreType.DMA((3,)),
        ],
        compiler_params=pltpu.CompilerParams(vmem_limit_bytes=66_200_000),
        name="tables",
    )(slots, pinv, ufac)


def exchange_kernel(
    tier, own, table_h, slots_h, blocks_h, pattern_h, rhs_h, ret, acc, where,
    table, slots, blocks, pattern, rhs, mask, send, fac, land, arr, res, back, in_sems,
    ring_ss, ring_rs, core_ss, core_rs, out_ss, out_rs, ret_ss, ret_rs,
):
    r = lax.axis_index("rows")
    c = lax.axis_index("cols")
    x = lax.rem(r, NX)
    z = lax.rem(lax.div(r, NX), NZ)
    y = lax.div(r, NX * NZ)
    me = y * NX + x

    def chip(yy, zz, xx):
        return (yy * NZ + zz) * NX + xx

    def peer(dy, dx):
        return lax.rem(y + dy, NY), lax.rem(x + dx, NX)

    above = lax.rem(z + 1, NZ)
    below = lax.rem(z + NZ - 1, NZ)

    barrier = pltpu.get_barrier_semaphore()
    for dy, dx in PEERS:
        py, px = peer(dy, dx)
        pl.semaphore_signal(barrier, inc=1, device_id=(chip(py, z, px), c), device_id_type=MESH)
    for zz in (above, below):
        pl.semaphore_signal(barrier, inc=1, device_id=(chip(y, zz, x), c), device_id_type=MESH)
    pl.semaphore_signal(barrier, inc=1, device_id=(r, 1 - c), device_id_type=MESH)

    fetches = [
        pltpu.make_async_copy(src, dst, in_sems.at[k])
        for k, (src, dst) in enumerate(
            ((table_h, table), (pattern_h, pattern), (rhs_h, rhs), (slots_h, slots), (blocks_h, blocks))
        )
    ]
    for fetch in fetches:
        fetch.start()
    pl.semaphore_wait(barrier, len(PEERS) + 3)

    def slot_at(i, d, away):
        zs = lax.rem(z - (1 - 2 * d) * (lax.div(i, 2) + away) + NZ, NZ)
        return SLOT_DEV * zs + lax.rem(i, 2)

    def slot_from(i, d):
        return slot_at(i, d, 1)

    def piece(k):
        at = (2 * c + k) * (PACKED // 4)
        return pl.ds(pl.multiple_of(at, PACKED // 4), PACKED // 4)

    def ring_copy(i, d, k, source=None):
        view = fac.at[slot_at(i, d, 0), piece(k), :]
        source = view if source is None else source.at[piece(k), :]
        return pltpu.make_async_remote_copy(
            source, view, ring_ss.at[d, k, i], ring_rs.at[d, k, i],
            device_id=(chip(y, jnp.where(d == 0, above, below), x), c), device_id_type=MESH,
        )

    def core_copy(i, d, k):
        view = fac.at[slot_from(i, d), piece(k), :]
        return pltpu.make_async_remote_copy(
            view, view, core_ss.at[d, k, i], core_rs.at[d, k, i],
            device_id=(r, 1 - c), device_id_type=MESH,
        )

    pieces = tuple((k, d) for k in range(2) for d in range(2))
    far_pieces = ((0, 0), (1, 1))

    lane = z * PLANE + me

    def pack(p):
        def one(m, carry):
            for a in range(2):
                f = table[RING_SLOTS + 2 * p + a, z * PLANE + m]
                for h in range(2):
                    b = blocks[h, f]
                    v = rhs[pl.ds(b, COLS, stride=ROW_BLOCKS), :] * mask[pl.ds(b, 1), :]
                    send[p, m, pl.ds(2 * a + h, COLS, stride=4), :] = v
            return carry

        lax.fori_loop(0, PLANE, one, 0, unroll=2)

    def rows_at(ref, p, m):
        return ref.at[p, pl.ds(pl.multiple_of(m * MSG, 8), MSG), :]

    def start_out(p):
        for dy, dx in PEERS:
            py, px = peer(dy, dx)
            pltpu.make_async_remote_copy(
                send.at[p, py * NX + px], rows_at(land, p, me), out_ss.at[p], out_rs.at[p],
                device_id=(chip(py, z, px), c), device_id_type=MESH,
            ).start()
        land[p, pl.ds(pl.multiple_of(me * MSG, 8), MSG), :] = send[p, me]

    def start_back(t):
        for dy, dx in PEERS:
            py, px = peer(dy, dx)
            pltpu.make_async_remote_copy(
                rows_at(back, t, py * NX + px), rows_at(ret, t, me), ret_ss.at[t], ret_rs.at[t],
                device_id=(chip(py, z, px), c), device_id_type=MESH,
            ).start()
        pltpu.make_async_copy(rows_at(back, t, me), rows_at(ret, t, me), ret_rs.at[t]).start()

    def wait_bytes(ref, p, n, sem):
        view = ref.at[p, pl.ds(0, n * MSG), :]
        pltpu.make_async_copy(view, view, sem).wait()

    row = lax.broadcasted_iota(jnp.int32, (BLOCK, BLOCK), 0)
    col = lax.broadcasted_iota(jnp.int32, (BLOCK, BLOCK), 1)

    def solve(o, factor):
        k = table[o, lane] & 255
        data = arr.at[k >> 1]
        second = (k & 1) == 1
        x0, x1 = (
            jnp.where(
                second,
                data[pl.ds(2 + h, PLANE * COLS, stride=4), :],
                data[pl.ds(h, PLANE * COLS, stride=4), :],
            )
            for h in range(2)
        )
        merged = factor[0:BLOCK, :]
        lower = jnp.where(row > col, merged, 0.0)
        upper = jnp.where(row < col, merged, 0.0)
        left = jnp.concatenate([lower, factor[BLOCK:PIV, :]], axis=0)
        first = product(nt, x0, left)
        y0 = x0 + first[:, :BLOCK]
        y1 = x1 + (first[:, BLOCK:] + product(nn, x1, upper))
        upd = product(nt, y0, factor[PIV : 2 * PIV, :]) + product(nt, y1, factor[2 * PIV : 3 * PIV, :])
        for h, v in enumerate((y0, y1, upd[:, :BLOCK], upd[:, BLOCK:])):
            res[o, pl.ds(h, PLANE * COLS, stride=4), :] = v

    def give_back(t):
        back[t] = res[table[t, lane] >> 16]
        start_back(t)

    for i in range(SLOT_DEV):
        for k, d in pieces:
            ring_copy(jnp.int32(i), d, k, own.at[i]).start()
    fetches[1].wait()
    for k in range(ROW_BLOCKS // BLOCK):
        on = pattern[:, k * BLOCK : (k + 1) * BLOCK].astype(jnp.float32)
        mask[k * BLOCK : (k + 1) * BLOCK, :] = jnp.broadcast_to(on, (BLOCK, BLOCK)).T
    fetches[0].wait()
    fetches[4].wait()
    fetches[2].wait()

    def out_step(p, carry):
        pack(p)
        start_out(p)
        return carry

    lax.fori_loop(0, (tier + 1) // 2, out_step, 0)

    def init(k, carry):
        on = mask[pl.ds(pl.multiple_of(8 * k, 8), 8), :]
        for j in range(COLS):
            v = rhs[pl.ds(pl.multiple_of(j * ROW_BLOCKS + 8 * k, 8), 8), :] * on
            acc[pl.ds(64 * k + j, 8, stride=8), :] = v
        return carry

    lax.fori_loop(0, ROW_BLOCKS // 8, init, 0, unroll=2)
    fetches[3].wait()

    fronts = slots.shape[0]

    def locate(f, carry):
        o, ring = sequence_of(slots[f], z)
        where[f] = (((table[o, z * PLANE + ring] >> 8) & 255) * PLANE + ring) * MSG
        for h in range(4):
            where[(h + 1) * fronts + f] = blocks[h, f] * 8
        return carry

    lax.fori_loop(0, fronts, locate, 0, unroll=4)

    early = jnp.where(z < NZ // 2, 1, 0)

    def forward(i, d):
        for k in range(2):
            ring_copy(i, d, k).wait_recv()

            @pl.when(i < jnp.where(d == k, FAR, FAR - 2))
            def _():
                ring_copy(i + 2, d, k).start()

            core_copy(i, d, k).start()

    def collect(i, d):
        for k in range(2):
            core_copy(i, d, k).wait_recv()

    def arrive(p):
        wait_bytes(land, p, PLANE - 1, out_rs.at[p])
        arr[p] = land[p]

    zero = jnp.int32(0)
    forward(zero, early)
    forward(zero, 1 - early)
    arrive(0)
    for a in range(2):
        solve(a, own.at[a])
    for t in range(first_position(tier, 2)):
        give_back(t)
    arrive(1)
    for a, d in enumerate((early, 1 - early)):
        collect(zero, d)
        solve(2 + a, fac.at[slot_from(zero, d)])
    for t in range(first_position(tier, 2), first_position(tier, 4)):
        give_back(t)

    def step(i, carry):
        p = i + 1
        for a, d in enumerate((early, 1 - early)):
            forward(i, d)
            if a == 0:

                @pl.when(p < (tier + 1) // 2)
                def _():
                    arrive(p)

            collect(i, d)
            solve(2 * p + a, fac.at[slot_from(i, d)])
            two = pairs_from(tier)
            t = 2 * p - (16 - tier) + a
            if a == 1:
                give_back(jnp.where(p < two, p - 1, t))
            elif two <= 2:
                give_back(t)
            else:

                @pl.when(p >= two)
                def _():
                    give_back(t)

        return carry

    lax.fori_loop(1, FAR, step, 0)

    if tier == 2 * PAIRS:
        arrive(PAIRS - 1)
    for i in range(FAR, FAR + 2):
        at = jnp.int32(i)
        for k, d in far_pieces:
            ring_copy(at, d, k).wait_recv()
            core_copy(at, d, k).start()
        for k, d in far_pieces:
            core_copy(at, d, k).wait_recv()
        solve(8 + i, fac.at[slot_from(at, 0)])
        give_back(first_position(tier, 8 + i))

    def drain(i, carry):
        for k, d in pieces:
            ring_copy(i, d, k).wait_send()
            core_copy(i, d, k).wait_send()
        return carry

    lax.fori_loop(0, FAR, drain, 0)
    for i in range(FAR, FAR + 2):
        for k, d in far_pieces:
            ring_copy(jnp.int32(i), d, k).wait_send()
            core_copy(jnp.int32(i), d, k).wait_send()

    def drain_out(p, carry):
        wait_bytes(arr, p, PLANE - 1, out_ss.at[p])
        return carry

    lax.fori_loop(0, (tier + 1) // 2, drain_out, 0)

    def drain_back(t, carry):
        wait_bytes(back, t, PLANE - 1, ret_ss.at[t])
        wait_bytes(back, t, PLANE, ret_rs.at[t])
        return carry

    lax.fori_loop(0, tier, drain_back, 0)


def exchange(tier, own, table, slots, blocks, pattern, rhs):
    vmem = pl.BlockSpec(memory_space=pltpu.VMEM)
    hbm = pl.BlockSpec(memory_space=pl.ANY)
    dma = pltpu.SemaphoreType.DMA
    f32 = jnp.float32
    return pl.pallas_call(
        functools.partial(exchange_kernel, tier),
        out_shape=(
            jax.ShapeDtypeStruct((RING_SLOTS, PLANE * MSG, BLOCK), f32),
            jax.ShapeDtypeStruct((ROW_BLOCKS * 8, BLOCK), f32),
            jax.ShapeDtypeStruct((5 * slots.shape[0],), jnp.int32),
        ),
        in_specs=[vmem] + [hbm] * 5,
        out_specs=(hbm, vmem, pl.BlockSpec(memory_space=pltpu.SMEM)),
        scratch_shapes=[
            pltpu.SMEM(table.shape, jnp.int32),
            pltpu.SMEM(slots.shape, jnp.int32),
            pltpu.SMEM(blocks.shape, jnp.int32),
            pltpu.VMEM(pattern.shape, jnp.int32),
            pltpu.VMEM(rhs.shape, f32),
            pltpu.VMEM((ROW_BLOCKS, BLOCK), f32),
            pltpu.VMEM((PAIRS, PLANE, MSG, BLOCK), f32),
            pltpu.VMEM((RING_SLOTS, PACKED, BLOCK), f32),
            pltpu.VMEM((PAIRS, PLANE * MSG, BLOCK), f32),
            pltpu.VMEM((PAIRS, PLANE * MSG, BLOCK), f32),
            pltpu.VMEM((RING_SLOTS, PLANE * MSG, BLOCK), f32),
            pltpu.VMEM((RING_SLOTS, PLANE * MSG, BLOCK), f32),
            dma((5,)),
            *[dma((2, 2, FAR + 2))] * 4,
            dma((PAIRS,)), dma((PAIRS,)), dma((RING_SLOTS,)), dma((RING_SLOTS,)),
        ],
        compiler_params=pltpu.CompilerParams(
            collective_id=TIERS.index(tier), has_side_effects=True, vmem_limit_bytes=36 * 1024 * 1024
        ),
        name=f"exchange_{tier}",
    )(own, table, slots, blocks, pattern, rhs)


def assemble_kernel(where, ret, acc_in, out_h, acc, out, sems):
    del acc_in
    fronts = where.shape[0] // 5

    def one_front(f, carry):
        at = pl.multiple_of(where[f], 8)
        for h in range(4):
            rows = pl.ds(pl.multiple_of(where[(h + 1) * fronts + f], 8), COLS)
            v = ret[pl.ds(at + h, COLS, stride=4), :]
            acc[rows, :] = v if h < 2 else acc[rows, :] - v
        return carry

    lax.fori_loop(0, fronts, one_front, 0, unroll=8)

    copies = []
    for j in range(COLS):

        def regroup(k, carry):
            rows = pl.ds(pl.multiple_of(j * ROW_BLOCKS + 8 * k, 8), 8)
            out[rows, :] = acc[pl.ds(64 * k + j, 8, stride=8), :]
            return carry

        lax.fori_loop(0, ROW_BLOCKS // 8, regroup, 0, unroll=8)
        rows = pl.ds(j * ROW_BLOCKS, ROW_BLOCKS)
        copies.append(pltpu.make_async_copy(out.at[rows, :], out_h.at[rows, :], sems.at[j]))
        copies[-1].start()
    for copy in copies:
        copy.wait()


def assemble(where, ret, acc):
    vmem = pl.BlockSpec(memory_space=pltpu.VMEM)
    smem = pl.BlockSpec(memory_space=pltpu.SMEM)
    shape = (COLS * ROW_BLOCKS, BLOCK)
    return pl.pallas_call(
        assemble_kernel,
        out_shape=(
            jax.ShapeDtypeStruct(shape, jnp.float32),
            jax.ShapeDtypeStruct(acc.shape, jnp.float32),
        ),
        in_specs=[smem, vmem, vmem],
        out_specs=(pl.BlockSpec(memory_space=pltpu.HBM), vmem),
        scratch_shapes=[pltpu.VMEM(shape, jnp.float32), pltpu.SemaphoreType.DMA((COLS,))],
        input_output_aliases={2: 1},
        compiler_params=pltpu.CompilerParams(vmem_limit_bytes=16 * 1024 * 1024),
        name="assemble",
    )(where, ret, acc)[0]


def branch(tier, own, table, slots, blocks, pattern, rhs):
    ret, acc, where = exchange(tier, own, table, slots, blocks, pattern, rhs)
    return assemble(where, ret.reshape(RING_SLOTS * PLANE * MSG, BLOCK), acc)


def on_device(rhs, pattern, front_blocks, front_slot, pivot_inverse, update_factor):
    shape = rhs.shape
    blocks = front_blocks.T
    table, own, tier = make_tables(front_slot, pivot_inverse, update_factor)
    out = lax.switch(
        tier[0],
        [functools.partial(branch, t) for t in TIERS],
        own, table, front_slot, blocks, pattern.T, rhs.reshape(COLS * ROW_BLOCKS, BLOCK),
    )
    return out.reshape(shape)


def solution(mesh):
    return jax.shard_map(
        on_device,
        mesh=mesh,
        in_specs=(
            P("cols", "rows", None),
            P(None, "cols"),
            P(),
            P(),
            P("rows", None, None),
            P("rows", None, None),
        ),
        out_specs=P("cols", "rows", None),
        check_vma=False,
    )
```

```python
import functools

import jax
import jax.numpy as jnp
from jax import lax
from jax.experimental import pallas as pl
from jax.experimental.pallas import tpu as pltpu
from jax.sharding import PartitionSpec as P

BLOCK = 128
PIV = 256
NX, NY, NZ = 4, 4, 8
PLANE = NX * NY
SLOT_DEV = 2
PAIRS = NZ
RING_SLOTS = NZ * SLOT_DEV
COLS = 6
ROW_BLOCKS = 384
MSG = COLS * 4
FAR = 6
PACKED = 768
MESH = pl.DeviceIdType.MESH
PEERS = (
    (2, 2), (2, 1), (2, 3), (1, 2), (3, 2), (1, 1), (3, 3), (1, 3),
    (3, 1), (0, 2), (2, 0), (0, 1), (1, 0), (0, 3), (3, 0),
)


def nt(a, b):
    return lax.dot_general(a, b, (((1,), (1,)), ((), ())), preferred_element_type=jnp.float32)


def nn(a, b):
    return lax.dot_general(a, b, (((1,), (0,)), ((), ())), preferred_element_type=jnp.float32)


def split(v):
    high = v.astype(jnp.bfloat16)
    low = (v - high.astype(jnp.float32)).astype(jnp.bfloat16)
    return high, low


def product(dot, x, w):
    xh, xl = split(x)
    wh, wl = split(w)
    both = dot(jnp.concatenate([xh, xl], axis=0), wh)
    n = x.shape[0]
    return both[:n] + (both[n:] + dot(xh, wl))


TIERS = (12, 13, 16)


def pairs_from(tier):
    return max(15 - tier, 0)


def first_position(tier, o):
    p, a = o // 2, o % 2
    start = max(2 * p - (16 - tier), p - 1, 0)
    return start + a if p >= pairs_from(tier) else start


def slot_in_sequence(o, z, ring):
    p, a = o >> 1, o & 1
    i = p - 1
    reach = (i >> 1) + 1
    edge = jnp.logical_or(p == 0, p == PAIRS - 1)
    lower = (a ^ jnp.where(z < NZ // 2, 1, 0)) == 0
    zs = jnp.where(p == 0, z, jnp.where(lower, z - reach, z + reach)) & (NZ - 1)
    sl = jnp.where(edge, a, i & 1)
    zs = jnp.where(p == PAIRS - 1, z + NZ // 2, zs) & (NZ - 1)
    return (((ring >> 2) * NZ + zs) * NX + (ring & (NX - 1))) * SLOT_DEV + sl


def sequence_of(slot, z):
    sl = slot & 1
    ring = ((slot >> 6) << 2) + ((slot >> 1) & 3)
    delta = (z - (slot >> 3)) & (NZ - 1)
    below = delta < NZ // 2
    o = 4 * jnp.where(below, delta, NZ - delta) - 2 + 2 * sl
    o = o + (jnp.where(below, 0, 1) ^ jnp.where(z < NZ // 2, 1, 0))
    o = jnp.where(delta == NZ // 2, 2 * (PAIRS - 1) + sl, o)
    return jnp.where(delta == 0, sl, o), ring


def tables_kernel(slots_h, pinv_h, ufac_h, table, own, tier_ref, slots, pinv, ufac, sems):
    fetches = [
        pltpu.make_async_copy(src, dst, sems.at[k])
        for k, (src, dst) in enumerate(((slots_h, slots), (pinv_h, pinv), (ufac_h, ufac)))
    ]
    for fetch in fetches:
        fetch.start()
    shape = (RING_SLOTS, 128)
    o_of = lax.broadcasted_iota(jnp.int32, shape, 0)
    lane = lax.broadcasted_iota(jnp.int32, shape, 1)
    slot_of = slot_in_sequence(o_of, lane >> 4, lane & 15)
    fetches[0].wait()

    def mark(f, code):
        for k in range(16):
            g = 16 * f + k
            code = jnp.where(slot_of == slots[g], 1 + g, code)
        return code

    code = lax.fori_loop(0, slots.shape[0] // 16, mark, jnp.zeros(shape, jnp.int32))
    used = code > 0
    count = jnp.zeros((1, 128), jnp.int32)
    ranks = []
    last = {t: jnp.full((1, 128), -1, jnp.int32) for t in TIERS}
    places = {t: [] for t in TIERS}
    for o in range(RING_SLOTS):
        on = used[o : o + 1]
        ranks.append(jnp.where(on, count, 0))
        count = count + on.astype(jnp.int32)
        for t in TIERS:
            last[t] = jnp.where(on, jnp.maximum(last[t] + 1, first_position(t, o)), last[t])
            places[t].append(jnp.where(on, last[t], 255))
    fits = [jnp.max(last[t]) < t for t in TIERS]
    tier = jnp.where(fits[0], 0, jnp.where(fits[1], 1, 2))
    place = {t: jnp.concatenate(places[t], axis=0) for t in TIERS}
    place = jnp.where(tier == 0, place[TIERS[0]], jnp.where(tier == 1, place[TIERS[1]], place[TIERS[2]]))
    holds = jnp.zeros(shape, jnp.int32)
    by_rank = jnp.zeros(shape, jnp.int32)
    for o in range(RING_SLOTS):
        holds = jnp.where(place[o : o + 1] == o_of, o, holds)
        mine = jnp.logical_and(used[o : o + 1], ranks[o] == o_of)
        by_rank = jnp.where(mine, code[o : o + 1] - 1, by_rank)
    table[0:RING_SLOTS, :] = jnp.concatenate(ranks, axis=0) + (place << 8) + (holds << 16)
    table[RING_SLOTS : 2 * RING_SLOTS, :] = by_rank
    tier_ref[0] = tier
    fetches[1].wait()
    fetches[2].wait()

    row = lax.broadcasted_iota(jnp.int32, (BLOCK, BLOCK), 0)
    col = lax.broadcasted_iota(jnp.int32, (BLOCK, BLOCK), 1)
    for s in range(SLOT_DEV):
        own[s, 0:BLOCK, :] = jnp.where(
            row > col, pinv[s, :BLOCK, :BLOCK], pinv[s, BLOCK:, BLOCK:].T
        )
        own[s, BLOCK : 2 * BLOCK, :] = pinv[s, BLOCK:, :BLOCK]
        own[s, PIV : 2 * PIV, :] = ufac[s, :, :BLOCK]
        own[s, 2 * PIV : 3 * PIV, :] = ufac[s, :, BLOCK:]


def make_tables(slots, pinv, ufac):
    hbm = pl.BlockSpec(memory_space=pltpu.HBM)
    vmem = pl.BlockSpec(memory_space=pltpu.VMEM)
    return pl.pallas_call(
        tables_kernel,
        out_shape=(
            jax.ShapeDtypeStruct((2 * RING_SLOTS, 128), jnp.int32),
            jax.ShapeDtypeStruct((SLOT_DEV, PACKED, BLOCK), jnp.float32),
            jax.ShapeDtypeStruct((1,), jnp.int32),
        ),
        in_specs=[hbm] * 3,
        out_specs=(vmem, vmem, pl.BlockSpec(memory_space=pltpu.SMEM)),
        scratch_shapes=[
            pltpu.SMEM(slots.shape, jnp.int32),
            pltpu.VMEM(pinv.shape, jnp.float32),
            pltpu.VMEM(ufac.shape, jnp.float32),
            pltpu.SemaphoreType.DMA((3,)),
        ],
        compiler_params=pltpu.CompilerParams(vmem_limit_bytes=66_200_000),
        name="tables",
    )(slots, pinv, ufac)


def exchange_kernel(
    tier, own, table_h, slots_h, blocks_h, pattern_h, rhs_h, ret, acc, where,
    table, slots, blocks, pattern, rhs, mask, send, fac, land, arr, res, back, in_sems,
    ring_ss, ring_rs, core_ss, core_rs, out_ss, out_rs, ret_ss, ret_rs,
):
    r = lax.axis_index("rows")
    c = lax.axis_index("cols")
    x = lax.rem(r, NX)
    z = lax.rem(lax.div(r, NX), NZ)
    y = lax.div(r, NX * NZ)
    me = y * NX + x

    def chip(yy, zz, xx):
        return (yy * NZ + zz) * NX + xx

    def peer(dy, dx):
        return lax.rem(y + dy, NY), lax.rem(x + dx, NX)

    above = lax.rem(z + 1, NZ)
    below = lax.rem(z + NZ - 1, NZ)

    barrier = pltpu.get_barrier_semaphore()
    for zz in (above, below):
        pl.semaphore_signal(barrier, inc=1, device_id=(chip(y, zz, x), c), device_id_type=MESH)
    for dy, dx in PEERS:
        py, px = peer(dy, dx)
        pl.semaphore_signal(barrier, inc=1, device_id=(chip(py, z, px), c), device_id_type=MESH)
    pl.semaphore_signal(barrier, inc=1, device_id=(r, 1 - c), device_id_type=MESH)

    fetches = [
        pltpu.make_async_copy(src, dst, in_sems.at[k])
        for k, (src, dst) in enumerate(
            ((table_h, table), (pattern_h, pattern), (rhs_h, rhs), (slots_h, slots), (blocks_h, blocks))
        )
    ]
    for fetch in fetches:
        fetch.start()
    pl.semaphore_wait(barrier, len(PEERS) + 3)

    def slot_at(i, d, away):
        zs = lax.rem(z - (1 - 2 * d) * (lax.div(i, 2) + away) + NZ, NZ)
        return SLOT_DEV * zs + lax.rem(i, 2)

    def slot_from(i, d):
        return slot_at(i, d, 1)

    def piece(k):
        at = (2 * c + k) * (PACKED // 4)
        return pl.ds(pl.multiple_of(at, PACKED // 4), PACKED // 4)

    def ring_copy(i, d, k, source=None):
        view = fac.at[slot_at(i, d, 0), piece(k), :]
        source = view if source is None else source.at[piece(k), :]
        return pltpu.make_async_remote_copy(
            source, view, ring_ss.at[d, k, i], ring_rs.at[d, k, i],
            device_id=(chip(y, jnp.where(d == 0, above, below), x), c), device_id_type=MESH,
        )

    def core_copy(i, d, k):
        view = fac.at[slot_from(i, d), piece(k), :]
        return pltpu.make_async_remote_copy(
            view, view, core_ss.at[d, k, i], core_rs.at[d, k, i],
            device_id=(r, 1 - c), device_id_type=MESH,
        )

    pieces = tuple((k, d) for k in range(2) for d in range(2))
    far_pieces = ((0, 0), (1, 1))

    lane = z * PLANE + me

    def pack(p):
        def one(m, carry):
            for a in range(2):
                f = table[RING_SLOTS + 2 * p + a, z * PLANE + m]
                for h in range(2):
                    b = blocks[h, f]
                    v = rhs[pl.ds(b, COLS, stride=ROW_BLOCKS), :] * mask[pl.ds(b, 1), :]
                    send[p, m, pl.ds(2 * a + h, COLS, stride=4), :] = v
            return carry

        lax.fori_loop(0, PLANE, one, 0, unroll=2)

    def rows_at(ref, p, m):
        return ref.at[p, pl.ds(pl.multiple_of(m * MSG, 8), MSG), :]

    def start_out(p):
        for dy, dx in PEERS:
            py, px = peer(dy, dx)
            pltpu.make_async_remote_copy(
                send.at[p, py * NX + px], rows_at(land, p, me), out_ss.at[p], out_rs.at[p],
                device_id=(chip(py, z, px), c), device_id_type=MESH,
            ).start()
        land[p, pl.ds(pl.multiple_of(me * MSG, 8), MSG), :] = send[p, me]

    def start_back(t):
        for dy, dx in PEERS:
            py, px = peer(dy, dx)
            pltpu.make_async_remote_copy(
                rows_at(back, t, py * NX + px), rows_at(ret, t, me), ret_ss.at[t], ret_rs.at[t],
                device_id=(chip(py, z, px), c), device_id_type=MESH,
            ).start()
        pltpu.make_async_copy(rows_at(back, t, me), rows_at(ret, t, me), ret_rs.at[t]).start()

    def wait_bytes(ref, p, n, sem):
        view = ref.at[p, pl.ds(0, n * MSG), :]
        pltpu.make_async_copy(view, view, sem).wait()

    row = lax.broadcasted_iota(jnp.int32, (BLOCK, BLOCK), 0)
    col = lax.broadcasted_iota(jnp.int32, (BLOCK, BLOCK), 1)

    def solve(o, factor):
        k = table[o, lane] & 255
        data = arr.at[k >> 1]
        second = (k & 1) == 1
        x0, x1 = (
            jnp.where(
                second,
                data[pl.ds(2 + h, PLANE * COLS, stride=4), :],
                data[pl.ds(h, PLANE * COLS, stride=4), :],
            )
            for h in range(2)
        )
        merged = factor[0:BLOCK, :]
        lower = jnp.where(row > col, merged, 0.0)
        upper = jnp.where(row < col, merged, 0.0)
        left = jnp.concatenate([lower, factor[BLOCK:PIV, :]], axis=0)
        first = product(nt, x0, left)
        y0 = x0 + first[:, :BLOCK]
        y1 = x1 + (first[:, BLOCK:] + product(nn, x1, upper))
        upd = product(nt, y0, factor[PIV : 2 * PIV, :]) + product(nt, y1, factor[2 * PIV : 3 * PIV, :])
        for h, v in enumerate((y0, y1, upd[:, :BLOCK], upd[:, BLOCK:])):
            res[o, pl.ds(h, PLANE * COLS, stride=4), :] = v

    def give_back(t):
        back[t] = res[table[t, lane] >> 16]
        start_back(t)

    for i in range(SLOT_DEV):
        for k, d in pieces:
            ring_copy(jnp.int32(i), d, k, own.at[i]).start()
    fetches[1].wait()
    for k in range(ROW_BLOCKS // BLOCK):
        on = pattern[:, k * BLOCK : (k + 1) * BLOCK].astype(jnp.float32)
        mask[k * BLOCK : (k + 1) * BLOCK, :] = jnp.broadcast_to(on, (BLOCK, BLOCK)).T
    fetches[0].wait()
    fetches[4].wait()
    fetches[2].wait()

    def out_step(p, carry):
        pack(p)
        start_out(p)
        return carry

    lax.fori_loop(0, (tier + 1) // 2, out_step, 0)

    def init(k, carry):
        on = mask[pl.ds(pl.multiple_of(8 * k, 8), 8), :]
        for j in range(COLS):
            v = rhs[pl.ds(pl.multiple_of(j * ROW_BLOCKS + 8 * k, 8), 8), :] * on
            acc[pl.ds(64 * k + j, 8, stride=8), :] = v
        return carry

    lax.fori_loop(0, ROW_BLOCKS // 8, init, 0, unroll=2)
    fetches[3].wait()

    fronts = slots.shape[0]

    def locate(f, carry):
        o, ring = sequence_of(slots[f], z)
        where[f] = (((table[o, z * PLANE + ring] >> 8) & 255) * PLANE + ring) * MSG
        for h in range(4):
            where[(h + 1) * fronts + f] = blocks[h, f] * 8
        return carry

    lax.fori_loop(0, fronts, locate, 0, unroll=4)

    early = jnp.where(z < NZ // 2, 1, 0)

    def forward(i, d):
        for k in range(2):
            ring_copy(i, d, k).wait_recv()

            @pl.when(i < jnp.where(d == k, FAR, FAR - 2))
            def _():
                ring_copy(i + 2, d, k).start()

            core_copy(i, d, k).start()

    def collect(i, d):
        for k in range(2):
            core_copy(i, d, k).wait_recv()

    def arrive(p):
        wait_bytes(land, p, PLANE - 1, out_rs.at[p])
        arr[p] = land[p]

    zero = jnp.int32(0)
    forward(zero, early)
    forward(zero, 1 - early)
    arrive(0)
    for a in range(2):
        solve(a, own.at[a])
    for t in range(first_position(tier, 2)):
        give_back(t)
    arrive(1)
    for a, d in enumerate((early, 1 - early)):
        collect(zero, d)
        solve(2 + a, fac.at[slot_from(zero, d)])
    for t in range(first_position(tier, 2), first_position(tier, 4)):
        give_back(t)

    def step(i, carry):
        p = i + 1
        for a, d in enumerate((early, 1 - early)):
            forward(i, d)
            if a == 0:

                @pl.when(p < (tier + 1) // 2)
                def _():
                    arrive(p)

            collect(i, d)
            solve(2 * p + a, fac.at[slot_from(i, d)])
            two = pairs_from(tier)
            t = 2 * p - (16 - tier) + a
            if a == 1:
                give_back(jnp.where(p < two, p - 1, t))
            elif two <= 2:
                give_back(t)
            else:

                @pl.when(p >= two)
                def _():
                    give_back(t)

        return carry

    lax.fori_loop(1, FAR, step, 0)

    if tier == 2 * PAIRS:
        arrive(PAIRS - 1)
    for i in range(FAR, FAR + 2):
        at = jnp.int32(i)
        for k, d in far_pieces:
            ring_copy(at, d, k).wait_recv()
            core_copy(at, d, k).start()
        for k, d in far_pieces:
            core_copy(at, d, k).wait_recv()
        solve(8 + i, fac.at[slot_from(at, 0)])
        give_back(first_position(tier, 8 + i))

    def drain(i, carry):
        for k, d in pieces:
            ring_copy(i, d, k).wait_send()
            core_copy(i, d, k).wait_send()
        return carry

    lax.fori_loop(0, FAR, drain, 0)
    for i in range(FAR, FAR + 2):
        for k, d in far_pieces:
            ring_copy(jnp.int32(i), d, k).wait_send()
            core_copy(jnp.int32(i), d, k).wait_send()

    def drain_out(p, carry):
        wait_bytes(arr, p, PLANE - 1, out_ss.at[p])
        return carry

    lax.fori_loop(0, (tier + 1) // 2, drain_out, 0)

    def drain_back(t, carry):
        wait_bytes(back, t, PLANE - 1, ret_ss.at[t])
        wait_bytes(back, t, PLANE, ret_rs.at[t])
        return carry

    lax.fori_loop(0, tier, drain_back, 0)


def exchange(tier, own, table, slots, blocks, pattern, rhs):
    vmem = pl.BlockSpec(memory_space=pltpu.VMEM)
    hbm = pl.BlockSpec(memory_space=pl.ANY)
    dma = pltpu.SemaphoreType.DMA
    f32 = jnp.float32
    return pl.pallas_call(
        functools.partial(exchange_kernel, tier),
        out_shape=(
            jax.ShapeDtypeStruct((RING_SLOTS, PLANE * MSG, BLOCK), f32),
            jax.ShapeDtypeStruct((ROW_BLOCKS * 8, BLOCK), f32),
            jax.ShapeDtypeStruct((5 * slots.shape[0],), jnp.int32),
        ),
        in_specs=[vmem] + [hbm] * 5,
        out_specs=(hbm, vmem, pl.BlockSpec(memory_space=pltpu.SMEM)),
        scratch_shapes=[
            pltpu.SMEM(table.shape, jnp.int32),
            pltpu.SMEM(slots.shape, jnp.int32),
            pltpu.SMEM(blocks.shape, jnp.int32),
            pltpu.VMEM(pattern.shape, jnp.int32),
            pltpu.VMEM(rhs.shape, f32),
            pltpu.VMEM((ROW_BLOCKS, BLOCK), f32),
            pltpu.VMEM((PAIRS, PLANE, MSG, BLOCK), f32),
            pltpu.VMEM((RING_SLOTS, PACKED, BLOCK), f32),
            pltpu.VMEM((PAIRS, PLANE * MSG, BLOCK), f32),
            pltpu.VMEM((PAIRS, PLANE * MSG, BLOCK), f32),
            pltpu.VMEM((RING_SLOTS, PLANE * MSG, BLOCK), f32),
            pltpu.VMEM((RING_SLOTS, PLANE * MSG, BLOCK), f32),
            dma((5,)),
            *[dma((2, 2, FAR + 2))] * 4,
            dma((PAIRS,)), dma((PAIRS,)), dma((RING_SLOTS,)), dma((RING_SLOTS,)),
        ],
        compiler_params=pltpu.CompilerParams(
            collective_id=TIERS.index(tier), has_side_effects=True, vmem_limit_bytes=36 * 1024 * 1024
        ),
        name=f"exchange_{tier}",
    )(own, table, slots, blocks, pattern, rhs)


def assemble_kernel(where, ret, acc_in, out_h, acc, out, sems):
    del acc_in
    fronts = where.shape[0] // 5

    def one_front(f, carry):
        at = pl.multiple_of(where[f], 8)
        for h in range(4):
            rows = pl.ds(pl.multiple_of(where[(h + 1) * fronts + f], 8), COLS)
            v = ret[pl.ds(at + h, COLS, stride=4), :]
            acc[rows, :] = v if h < 2 else acc[rows, :] - v
        return carry

    lax.fori_loop(0, fronts, one_front, 0, unroll=8)

    copies = []
    for j in range(COLS):

        def regroup(k, carry):
            rows = pl.ds(pl.multiple_of(j * ROW_BLOCKS + 8 * k, 8), 8)
            out[rows, :] = acc[pl.ds(64 * k + j, 8, stride=8), :]
            return carry

        lax.fori_loop(0, ROW_BLOCKS // 8, regroup, 0, unroll=8)
        rows = pl.ds(j * ROW_BLOCKS, ROW_BLOCKS)
        copies.append(pltpu.make_async_copy(out.at[rows, :], out_h.at[rows, :], sems.at[j]))
        copies[-1].start()
    for copy in copies:
        copy.wait()


def assemble(where, ret, acc):
    vmem = pl.BlockSpec(memory_space=pltpu.VMEM)
    smem = pl.BlockSpec(memory_space=pltpu.SMEM)
    shape = (COLS * ROW_BLOCKS, BLOCK)
    return pl.pallas_call(
        assemble_kernel,
        out_shape=(
            jax.ShapeDtypeStruct(shape, jnp.float32),
            jax.ShapeDtypeStruct(acc.shape, jnp.float32),
        ),
        in_specs=[smem, vmem, vmem],
        out_specs=(pl.BlockSpec(memory_space=pltpu.HBM), vmem),
        scratch_shapes=[pltpu.VMEM(shape, jnp.float32), pltpu.SemaphoreType.DMA((COLS,))],
        input_output_aliases={2: 1},
        compiler_params=pltpu.CompilerParams(vmem_limit_bytes=16 * 1024 * 1024),
        name="assemble",
    )(where, ret, acc)[0]


def branch(tier, own, table, slots, blocks, pattern, rhs):
    ret, acc, where = exchange(tier, own, table, slots, blocks, pattern, rhs)
    return assemble(where, ret.reshape(RING_SLOTS * PLANE * MSG, BLOCK), acc)


def on_device(rhs, pattern, front_blocks, front_slot, pivot_inverse, update_factor):
    shape = rhs.shape
    blocks = front_blocks.T
    table, own, tier = make_tables(front_slot, pivot_inverse, update_factor)
    out = lax.switch(
        tier[0],
        [functools.partial(branch, t) for t in TIERS],
        own, table, front_slot, blocks, pattern.T, rhs.reshape(COLS * ROW_BLOCKS, BLOCK),
    )
    return out.reshape(shape)


def solution(mesh):
    return jax.shard_map(
        on_device,
        mesh=mesh,
        in_specs=(
            P("cols", "rows", None),
            P(None, "cols"),
            P(),
            P(),
            P("rows", None, None),
            P("rows", None, None),
        ),
        out_specs=P("cols", "rows", None),
        check_vma=False,
    )
```
